32 devices in a mesh: member: 2 (over core), tp: 16 (over z, y, x).
Axes of the slice: x: 2, y: 2, z: 4, core: 2. Of those that a mesh axis runs over, the one named last changes fastest.
Arguments:
- stream_in: bfloat16 [512, 4096], P(('member', 'tp')), may hold values from -6 to 6
- kv_cache: bfloat16 [512, 512, 2048], P(('member', 'tp')), may hold values from -400 to 400
- lengths: int32 [128], replicated, may hold values from 1 to 512
- targets: int32 [128], replicated, may hold values from 0 to 65535
- norm_gains: float32 [3, 4096], replicated, may hold values from 0.1 to 1.9
- w_qkv: bfloat16 [4096, 6144], P(None, 'tp'), may hold values from -0.09375 to 0.09375
- w_out: bfloat16 [4096, 4096], P('tp'), may hold values from -0.09375 to 0.09375
- w_gate_up: bfloat16 [2, 4096, 14336], P(None, None, 'tp'), may hold values from -0.09375 to 0.09375
- w_down: bfloat16 [14336, 4096], P('tp'), may hold values from -0.046875 to 0.046875
- lm_head: bfloat16 [4096, 65536], P(None, 'tp'), may hold values from -300 to 300
- fast_in: float32 [4, 2, 4096], P('member'), may hold values from 0.1 to 1.9
- fast_hidden: float32 [4, 3, 14336], P('member', None, 'tp'), may hold values from 0.1 to 1.9
- fast_out: float32 [4, 4096], P('member'), may hold values from 0.1 to 1.9
Outputs:
- mean_logits: bfloat16 [128, 65536], P(None, 'tp')
- token_logprob: float32 [128], replicated
The draws below stay inside these ranges and needn't reach their ends.
Inputs may be any that keep to these rules, and one draw needn't show every extreme that they name: lengths is the same for all members.
All inputs are finite; a program needn't handle non-finite values.
Results may differ from the reference program's by a relative error of at most 0.02.
Values may be sent and summed in bfloat16 or wider, within the bound.
A program may use at most 192 MiB of HBM per device.

```python
import math
import jax
import jax.numpy as jnp
import numpy as np
from jax import lax

D = 4096
HEADS = 32
KV = 8
HD = 128
FF = 14336
VOCAB = 65536
B = 128
CACHE = 512
MEMBERS = 4


def draw_kv_cache(key, part):
    row_total = MEMBERS * B
    array_shape = (row_total, CACHE, 2 * KV * HD)
    key_main = jax.random.fold_in(key, 11)
    raw_draw = jnp.clip(jax.random.normal(key_main, array_shape, jnp.float32), -6.0, 6.0)
    return raw_draw.astype(jnp.bfloat16)


def draw_lm_head(key, part):
    array_shape = (D, VOCAB)
    key_main = jax.random.fold_in(key, 61)
    spread_scale = 3.0 / math.sqrt(D)
    result = jnp.clip(jax.random.normal(key_main, array_shape, jnp.float32) * spread_scale, -6.0 * spread_scale, 6.0 * spread_scale)
    return result.astype(jnp.bfloat16)


def with_ends(values, stream_key, low, largest):
    longest = values.shape.index(max(values.shape))
    spots = []
    for shift in (0, 1):
        where = [jax.random.randint(jax.random.fold_in(stream_key, axis), (), 0, length) for axis, length in enumerate(values.shape)]
        where[longest] = (where[longest] + shift) % values.shape[longest]
        spots.append(tuple(where))
    return values.at[spots[0]].set(low).at[spots[1]].set(largest)


def shard_levels(own_key, shape, shards, least, high):
    def one(axis_at, blocks):
        steps = jax.random.uniform(jax.random.fold_in(jax.random.fold_in(own_key, 6), axis_at), (blocks,), jnp.float32, least / len(shards), high / len(shards))
        return jnp.repeat(jnp.exp(steps), shape[axis_at] // blocks).reshape((-1,) + (1,) * (len(shape) - axis_at - 1))

    factor_of = one(*shards[0])
    for cut in shards[1:]:
        factor_of = factor_of * one(*cut)
    return factor_of


def rank_bounds(amount, skew):
    portions = [(1 << 20) // math.isqrt(grade ** skew) + 1 for grade in range(1, amount + 1)]
    deviation = 1 + sum(portions) // (1 << 30)
    return np.cumsum(np.array([max(1, weight // deviation) for weight in portions]))


def skewed_ids(stream_key, shape, number_of, slope):
    grid = rank_bounds(number_of, slope)
    lot = jax.random.randint(jax.random.fold_in(stream_key, 1), shape, 0, int(grid[number_of - 1]))
    grade = jnp.searchsorted(jnp.asarray(grid, jnp.int32), lot, side="right")
    return jax.random.permutation(jax.random.fold_in(stream_key, 2), number_of)[grade].astype(jnp.int32)


def noise(rng, shape, scale, most, cuts=(), held_as=jnp.bfloat16):
    values = scale * jax.random.normal(rng, shape, jnp.float32)
    if cuts:
        values = values * shard_levels(rng, shape, cuts, -0.22, 0.18)
    return jnp.clip(values, -most, most).astype(held_as)


def setup_inputs(seed: int = 0) -> dict:
    keys = jax.random.split(jax.random.key(seed), 14)
    return {
        "stream_in": noise(keys[0], (MEMBERS * B, D), 1.0, 6.0, ((0, 32),)),
        "kv_cache": draw_kv_cache(jax.random.fold_in(keys[13], 71), 0),
        "lengths": with_ends(jax.random.randint(keys[2], (B,), 1, CACHE + 1), jax.random.fold_in(keys[2], 1), 1, CACHE).astype(jnp.int32),
        "targets": with_ends(skewed_ids(keys[3], (B,), VOCAB, 2), jax.random.fold_in(keys[3], 3), 0, VOCAB - 1).astype(jnp.int32),
        "norm_gains": jnp.clip(1.0 + 0.18 * jax.random.normal(keys[4], (3, D), jnp.float32), 0.1, 1.9),
        "w_qkv": noise(keys[5], (D, (HEADS + 2 * KV) * HD), D ** -0.5, 0.09375, ((1, 16),)),
        "w_out": noise(keys[6], (HEADS * HD, D), (HEADS * HD) ** -0.5, 0.09375, ((0, 16),)),
        "w_gate_up": noise(keys[7], (2, D, FF), D ** -0.5, 0.09375, ((2, 16),)),
        "w_down": noise(keys[8], (FF, D), FF ** -0.5, 0.046875, ((0, 16),)),
        "lm_head": draw_lm_head(jax.random.fold_in(keys[13], 71), 0),
        "fast_in": jnp.clip(1.0 + 0.18 * jax.random.normal(keys[10], (MEMBERS, 2, D), jnp.float32), 0.1, 1.9),
        "fast_hidden": jnp.clip(1.0 + 0.18 * jax.random.normal(keys[11], (MEMBERS, 3, FF), jnp.float32), 0.1, 1.9),
        "fast_out": jnp.clip(1.0 + 0.18 * jax.random.normal(keys[12], (MEMBERS, D), jnp.float32), 0.1, 1.9),
    }


ROPE_BASE = 500000.0

def rms_norm(values_in, gain):
    return values_in * lax.rsqrt(lax.optimization_barrier(jnp.mean(values_in * values_in, axis=-1, keepdims=True)) + 1e-05) * gain

def rotate(values_in, positions):
    half_dim = values_in.shape[-1] // 2
    frequency = ROPE_BASE ** (-jnp.arange(half_dim, dtype=jnp.float32) * 2.0 / values_in.shape[-1])
    angles = positions.astype(jnp.float32)[:, None, None] * frequency[None, None, :]
    lower_half = values_in[..., :half_dim]
    upper_half = values_in[..., half_dim:]
    return jnp.concatenate([lower_half * jnp.cos(angles) - upper_half * jnp.sin(angles), upper_half * jnp.cos(angles) + lower_half * jnp.sin(angles)], axis=-1)

def attend(projected, cache_rows, positions):
    row_count = projected.shape[0]
    head_cols = HEADS * HD
    kv_cols = KV * HD
    queries = rotate(projected[:, :head_cols].astype(jnp.float32).reshape(row_count, HEADS, HD), positions).astype(jnp.bfloat16)
    new_key = rotate(projected[:, head_cols:head_cols + kv_cols].astype(jnp.float32).reshape(row_count, KV, HD), positions).astype(jnp.bfloat16)
    new_value = projected[:, head_cols + kv_cols:].reshape(row_count, KV, HD)
    cache_keys = cache_rows[:, :, :kv_cols].reshape(row_count, CACHE, KV, HD)
    cache_values = cache_rows[:, :, kv_cols:].reshape(row_count, CACHE, KV, HD)
    grouped = queries.reshape(row_count, KV, HEADS // KV, HD).astype(jnp.float32)
    inv_root = HD ** (-0.5)
    cached = jnp.einsum('rkgd,rckd->rkgc', grouped, cache_keys.astype(jnp.float32)) * inv_root
    fresh = jnp.einsum('rkgd,rkd->rkg', grouped, new_key.astype(jnp.float32)) * inv_root
    in_cache = jnp.arange(CACHE)[None, :] < positions[:, None]
    cached = jnp.where(in_cache[:, None, None, :], cached, -1e+30)
    peak = jnp.maximum(lax.optimization_barrier(jnp.max(cached, axis=-1)), fresh)
    weights = jnp.exp(cached - peak[..., None])
    fresh_w = jnp.exp(fresh - peak)
    total_sum = lax.optimization_barrier(jnp.sum(weights, axis=-1)) + fresh_w
    probs = (weights / total_sum[..., None]).astype(jnp.bfloat16)
    fresh_p = (fresh_w / total_sum).astype(jnp.bfloat16)
    result = jnp.einsum('rkgc,rckd->rkgd', probs.astype(jnp.float32), cache_values.astype(jnp.float32))
    result = result + fresh_p.astype(jnp.float32)[..., None] * new_value.astype(jnp.float32)[:, :, None, :]
    return result.reshape(row_count, HEADS * HD).astype(jnp.bfloat16)

def reference(stream_in, kv_cache, lengths, targets, norm_gains, w_qkv, w_out, w_gate_up, w_down, lm_head, fast_in, fast_hidden, fast_out):
    row_count = stream_in.shape[0]
    positions = jnp.tile(lengths, MEMBERS).astype(jnp.int32)
    attn_in = rms_norm(stream_in.astype(jnp.float32), norm_gains[0]).astype(jnp.bfloat16)
    projected = jnp.dot(attn_in, w_qkv, preferred_element_type=jnp.float32).astype(jnp.bfloat16)
    blocks = lax.map(lambda block_item: attend(block_item[0], block_item[1], block_item[2]), (projected.reshape(row_count // 8, 8, -1), kv_cache.reshape(row_count // 8, 8, CACHE, 2 * KV * HD), positions.reshape(row_count // 8, 8)))
    attended = blocks.reshape(row_count, HEADS * HD)
    middle = (stream_in.astype(jnp.float32) + jnp.dot(attended, w_out, preferred_element_type=jnp.float32)).astype(jnp.bfloat16)
    ffn_in = rms_norm(middle.astype(jnp.float32), norm_gains[1]).astype(jnp.bfloat16)
    grouped = ffn_in.astype(jnp.float32).reshape(MEMBERS, B, D)
    gate_in = (grouped * fast_in[:, 0][:, None, :]).astype(jnp.bfloat16).reshape(row_count, D)
    up_in = (grouped * fast_in[:, 1][:, None, :]).astype(jnp.bfloat16).reshape(row_count, D)
    gate_act = jnp.dot(gate_in, w_gate_up[0], preferred_element_type=jnp.float32).reshape(MEMBERS, B, FF) * fast_hidden[:, 0][:, None, :]
    up_act = jnp.dot(up_in, w_gate_up[1], preferred_element_type=jnp.float32).reshape(MEMBERS, B, FF) * fast_hidden[:, 1][:, None, :]
    hidden = (jax.nn.silu(gate_act) * up_act * fast_hidden[:, 2][:, None, :]).astype(jnp.bfloat16).reshape(row_count, FF)
    down_sum = jnp.dot(hidden, w_down, preferred_element_type=jnp.float32).reshape(MEMBERS, B, D) * fast_out[:, None, :]
    layer_out = (middle.astype(jnp.float32).reshape(MEMBERS, B, D) + down_sum).astype(jnp.bfloat16).reshape(row_count, D)
    final_in = rms_norm(layer_out.astype(jnp.float32), norm_gains[2]).astype(jnp.bfloat16)
    logits = jnp.dot(final_in, lm_head, preferred_element_type=jnp.float32)
    mean_logit = lax.optimization_barrier(jnp.sum(logits.reshape(MEMBERS, B, VOCAB), axis=0)) / MEMBERS
    peak = lax.optimization_barrier(jnp.max(mean_logit, axis=-1))
    log_total = peak + jnp.log(lax.optimization_barrier(jnp.sum(jnp.exp(mean_logit - peak[:, None]), axis=-1)))
    target_logit = lax.optimization_barrier(jnp.sum(jnp.where(jnp.arange(VOCAB)[None, :] == targets[:, None], mean_logit, 0.0), axis=-1))
    return (mean_logit.astype(jnp.bfloat16), target_logit - log_total)
```

```python
import functools
from types import SimpleNamespace

import jax
import jax.numpy as jnp
from jax import lax
from jax.experimental import pallas as pl
from jax.experimental.pallas import tpu as pltpu
from jax.sharding import PartitionSpec as P

HEADS = 32
KV = 8
HD = 128
CACHE = 512


ROPE_BASE = 500000.0


def rms_norm(values_in, gain):
    return (
        values_in
        * lax.rsqrt(jnp.mean(values_in * values_in, axis=-1, keepdims=True) + 1e-05)
        * gain
    )


def rotate(values_in, positions):
    half_dim = values_in.shape[-1] // 2
    frequency = ROPE_BASE ** (-jnp.arange(half_dim, dtype=jnp.float32) * 2.0 / values_in.shape[-1])
    angles = positions.astype(jnp.float32)[:, None, None] * frequency[None, None, :]
    lower_half = values_in[..., :half_dim]
    upper_half = values_in[..., half_dim:]
    return jnp.concatenate(
        [
            lower_half * jnp.cos(angles) - upper_half * jnp.sin(angles),
            upper_half * jnp.cos(angles) + lower_half * jnp.sin(angles),
        ],
        axis=-1,
    )


def attend(projected, cache_rows, positions):
    row_count = projected.shape[0]
    head_cols = HEADS * HD
    kv_cols = KV * HD
    queries = rotate(
        projected[:, :head_cols].astype(jnp.float32).reshape(row_count, HEADS, HD), positions
    ).astype(jnp.bfloat16)
    new_key = rotate(
        projected[:, head_cols : head_cols + kv_cols]
        .astype(jnp.float32)
        .reshape(row_count, KV, HD),
        positions,
    ).astype(jnp.bfloat16)
    new_value = projected[:, head_cols + kv_cols :].reshape(row_count, KV, HD)
    cache_keys = cache_rows[:, :, :kv_cols].reshape(row_count, CACHE, KV, HD)
    cache_values = cache_rows[:, :, kv_cols:].reshape(row_count, CACHE, KV, HD)
    grouped = queries.reshape(row_count, KV, HEADS // KV, HD)
    inv_root = HD ** (-0.5)
    cached = (
        jnp.einsum("rkgd,rckd->rkgc", grouped, cache_keys, preferred_element_type=jnp.float32)
        * inv_root
    )
    fresh = (
        jnp.einsum("rkgd,rkd->rkg", grouped, new_key, preferred_element_type=jnp.float32) * inv_root
    )
    in_cache = jnp.arange(CACHE)[None, :] < positions[:, None]
    cached = jnp.where(in_cache[:, None, None, :], cached, -1e30)
    peak = jnp.maximum(jnp.max(cached, axis=-1), fresh)
    weights = jnp.exp(cached - peak[..., None])
    fresh_w = jnp.exp(fresh - peak)
    total_sum = jnp.sum(weights, axis=-1) + fresh_w
    probs = (weights / total_sum[..., None]).astype(jnp.bfloat16)
    fresh_p = (fresh_w / total_sum).astype(jnp.bfloat16)
    result = jnp.einsum("rkgc,rckd->rkgd", probs, cache_values, preferred_element_type=jnp.float32)
    result = (
        result
        + fresh_p.astype(jnp.float32)[..., None] * new_value.astype(jnp.float32)[:, :, None, :]
    )
    return result.reshape(row_count, HEADS * HD).astype(jnp.bfloat16)


def plain_body(
    stream_in,
    kv_cache,
    lengths,
    targets,
    norm_gains,
    w_qkv,
    w_out,
    w_gate_up,
    w_down,
    lm_head,
    fast_in,
    fast_hidden,
    fast_out,
):
    tp_count = lax.axis_size("tp")
    tp_rank = lax.axis_index("tp")
    mem_dev = fast_in.shape[0]
    batch_rows = lengths.shape[0]
    own_rows = stream_in.shape[0]
    all_rows = own_rows * tp_count
    width = stream_in.shape[1]
    first_row = tp_rank * own_rows
    positions = lax.dynamic_slice_in_dim(lengths, first_row % batch_rows, own_rows, 0)
    own_member = first_row // batch_rows
    own_scale = lax.dynamic_index_in_dim(fast_out, own_member, 0, keepdims=True)
    own_normed = rms_norm(stream_in.astype(jnp.float32), norm_gains[0]).astype(jnp.bfloat16)
    attn_in = lax.all_gather(own_normed, "tp", axis=0, tiled=True)
    projected = jnp.dot(attn_in, w_qkv, preferred_element_type=jnp.float32).astype(jnp.bfloat16)
    row_major = lax.all_to_all(projected, "tp", split_axis=0, concat_axis=1, tiled=True)
    attended = attend(row_major, kv_cache, positions)
    head_major = lax.all_to_all(attended, "tp", split_axis=1, concat_axis=0, tiled=True)
    picked = head_major
    attn_sum = lax.psum_scatter(
        jnp.dot(picked, w_out, preferred_element_type=jnp.float32),
        "tp",
        scatter_dimension=0,
        tiled=True,
    )
    middle = (stream_in.astype(jnp.float32) + attn_sum).astype(jnp.bfloat16)
    own_ffn = rms_norm(middle.astype(jnp.float32), norm_gains[1]).astype(jnp.bfloat16)
    ffn_in = lax.all_gather(own_ffn, "tp", axis=0, tiled=True)
    grouped = ffn_in.astype(jnp.float32).reshape(mem_dev, batch_rows, width)
    gate_in = (grouped * fast_in[:, 0][:, None, :]).astype(jnp.bfloat16).reshape(all_rows, width)
    up_in = (grouped * fast_in[:, 1][:, None, :]).astype(jnp.bfloat16).reshape(all_rows, width)
    hidden_cols = w_gate_up.shape[2]
    gate_act = (
        jnp.dot(gate_in, w_gate_up[0], preferred_element_type=jnp.float32).reshape(
            mem_dev, batch_rows, hidden_cols
        )
        * fast_hidden[:, 0][:, None, :]
    )
    up_act = (
        jnp.dot(up_in, w_gate_up[1], preferred_element_type=jnp.float32).reshape(
            mem_dev, batch_rows, hidden_cols
        )
        * fast_hidden[:, 1][:, None, :]
    )
    hidden = (
        (jax.nn.silu(gate_act) * up_act * fast_hidden[:, 2][:, None, :])
        .astype(jnp.bfloat16)
        .reshape(all_rows, hidden_cols)
    )
    picked = hidden
    down_sum = lax.psum_scatter(
        jnp.dot(picked, w_down, preferred_element_type=jnp.float32),
        "tp",
        scatter_dimension=0,
        tiled=True,
    )
    layer_out = (middle.astype(jnp.float32) + down_sum * own_scale).astype(jnp.bfloat16)
    own_final = rms_norm(layer_out.astype(jnp.float32), norm_gains[2]).astype(jnp.bfloat16)
    final_in = lax.all_gather(own_final, "tp", axis=0, tiled=True)
    logits = jnp.dot(final_in, lm_head, preferred_element_type=jnp.float32)
    vocab_cols = lm_head.shape[1]
    member_total = jnp.sum(logits.reshape(mem_dev, batch_rows, vocab_cols), axis=0)
    member_count = mem_dev * lax.axis_size("member")
    mean_logit = (
        lax.psum(member_total.astype(jnp.bfloat16), "member").astype(jnp.float32) / member_count
    )
    column_ids = tp_rank * vocab_cols + jnp.arange(vocab_cols)
    target_part = jnp.sum(
        jnp.where(column_ids[None, :] == targets[:, None], mean_logit, 0.0), axis=-1
    )
    local_peak = jnp.max(mean_logit, axis=-1)
    peak = lax.pmax(local_peak, "tp")
    exp_total, target_logit = lax.psum(
        (jnp.sum(jnp.exp(mean_logit - peak[:, None]), axis=-1), target_part), "tp"
    )
    token_logprob = target_logit - (peak + jnp.log(exp_total))
    return (mean_logit.astype(jnp.bfloat16), token_logprob)


BF16 = jnp.bfloat16
F32 = jnp.float32
DMA = pltpu.SemaphoreType.DMA
QUAD = 4


def norm_rows(values_in, gain):
    return (
        values_in
        * lax.rsqrt(jnp.mean(values_in * values_in, axis=-1, keepdims=True) + 1e-05)
        * gain
    )


class Place:
    def __init__(self, lines):
        self.tp = lax.axis_index("tp")
        self.member = lax.axis_index("member")
        self.lines = lines
        self.quad = lax.rem(self.tp, QUAD)
        self.line = self.tp // QUAD
        self.quad_x = self.quad + 1 - 2 * lax.rem(self.quad, 2)
        self.quad_y = lax.rem(self.quad + 2, QUAD)
        self.quad_d = self.quad_x + self.quad_y - self.quad
        self.to_x = {"tp": self.line * QUAD + self.quad_x}
        self.to_y = {"tp": self.line * QUAD + self.quad_y}

    def line_at(self, step):
        return lax.rem(self.line + step + self.lines, self.lines)

    def to_line(self, step):
        return {"tp": self.line_at(step) * QUAD + self.quad}


def remote(src, dst, send_sem, recv_sem, device):
    copy = pltpu.make_async_remote_copy(
        src_ref=src,
        dst_ref=dst,
        send_sem=send_sem,
        recv_sem=recv_sem,
        device_id=device,
        device_id_type=pl.DeviceIdType.MESH,
    )
    copy.start()
    return copy


NT = (((1,), (1,)), ((), ()))
CHUNKS = 2


class Gather:
    def __init__(self, place, buf, rows, spans, sems):
        self.place, self.buf, self.rows, self.spans = place, buf, rows, spans
        self.sends, self.recvs = sems
        self.copies = {}

    def at(self, step, quad, start, width):
        index = self.place.line_at(step) * QUAD + quad
        rows = pl.ds(pl.multiple_of(index * self.rows, self.rows), self.rows)
        return self.buf.at[rows, pl.ds(start, width)]

    def send(self, kind, k, c, block, device):
        self.copies[kind, k, c] = remote(
            block, block, self.sends.at[kind, k, c], self.recvs.at[kind, k, c], device
        )

    def start(self):
        place = self.place
        for c, (start, width) in enumerate(self.spans):
            mine = self.at(0, place.quad, start, width)
            for k in range(1, place.lines):
                self.send(0, k, c, mine, place.to_line(k))
            self.send(1, 0, c, mine, place.to_x)
            self.send(2, 0, c, mine, place.to_y)

    def spread(self, c):
        place = self.place
        for k in range(1, place.lines):
            self.copies[0, k, c].wait_recv()
            block = self.at(-k, place.quad, *self.spans[c])
            self.send(1, k, c, block, place.to_x)
            self.send(2, k, c, block, place.to_y)

    def relay(self, c):
        place = self.place
        start, width = self.spans[c]
        half = width // 2
        for k in range(place.lines):
            self.copies[1, k, c].wait_recv()
            self.send(3, k, c, self.at(-k, place.quad_x, start, half), place.to_y)
            self.copies[2, k, c].wait_recv()
            self.send(4, k, c, self.at(-k, place.quad_y, start + half, half), place.to_x)

    def arrive(self, c):
        for k in range(self.place.lines):
            self.copies[3, k, c].wait_recv()
            self.copies[4, k, c].wait_recv()

    def run(self, compute):
        count = len(self.spans)
        self.start()
        self.spread(0)
        for c in range(count):
            if c + 1 < count:
                self.spread(c + 1)
            self.relay(c)
            if c:
                self.arrive(c - 1)
                compute(*self.spans[c - 1])
        self.arrive(count - 1)
        compute(*self.spans[count - 1])
        for copy in self.copies.values():
            copy.wait_send()


class Reduce:
    def __init__(self, place, part, total, rows, spans, sems, bufs):
        self.place, self.part, self.total = place, part, total
        self.rows, self.spans = rows, spans
        self.sends, self.recvs = sems
        self.got_dx, self.got_dy, self.put_x, self.put_y = bufs[:4]
        self.got_x, self.got_y, self.put_z, self.got_z = bufs[4:]
        self.steps = list(range(1, place.lines)) + [0]
        self.copies = {}

    def at(self, step, quad):
        index = self.place.line_at(step) * QUAD + quad
        return pl.ds(pl.multiple_of(index * self.rows, self.rows), self.rows)

    def send(self, kind, k, c, src, dst, device):
        self.copies[kind, k, c] = remote(
            src, dst, self.sends.at[kind, k, c], self.recvs.at[kind, k, c], device
        )

    def halves(self, c):
        start, width = self.spans[c]
        return pl.ds(start, width // 2), pl.ds(start + width // 2, width // 2)

    def direct(self, c):
        place, part = self.place, self.part
        low, high = self.halves(c)
        for k in self.steps:
            diag = self.at(k, place.quad_d)
            self.send(0, k, c, part.at[diag, high], self.got_dx.at[k, :, low_of(c, high)], place.to_x)
            self.send(1, k, c, part.at[diag, low], self.got_dy.at[k, :, low_of(c, low)], place.to_y)
        for k in self.steps:
            self.send(2, k, c, part.at[self.at(k, place.quad_x), high], self.got_x.at[k, :, high], place.to_x)
            self.send(3, k, c, part.at[self.at(k, place.quad_y), low], self.got_y.at[k, :, low], place.to_y)

    def follow(self, c):
        place, part = self.place, self.part
        low, high = self.halves(c)
        packed = low_of(c, low)
        for k in self.steps:
            self.copies[1, k, c].wait_recv()
            self.put_x[k, :, packed] = (
                part[self.at(k, place.quad_x), low].astype(F32)
                + self.got_dy[k, :, packed].astype(F32)
            ).astype(BF16)
            self.send(4, k, c, self.put_x.at[k, :, packed], self.got_x.at[k, :, low], place.to_x)
            self.copies[0, k, c].wait_recv()
            self.put_y[k, :, packed] = (
                part[self.at(k, place.quad_y), high].astype(F32)
                + self.got_dx[k, :, packed].astype(F32)
            ).astype(BF16)
            self.send(5, k, c, self.put_y.at[k, :, packed], self.got_y.at[k, :, high], place.to_y)

    def settle(self, c):
        place, part = self.place, self.part
        span = pl.ds(*self.spans[c])
        for k in self.steps:
            for kind in (2, 3, 4, 5):
                self.copies[kind, k, c].wait_recv()
            quad_sum = (
                part[self.at(k, place.quad), span].astype(F32)
                + self.got_x[k, :, span].astype(F32)
                + self.got_y[k, :, span].astype(F32)
            )
            if k:
                self.put_z[k, :, span] = quad_sum.astype(BF16)
                self.send(6, k, c, self.put_z.at[k, :, span], self.got_z.at[k, :, span], place.to_line(k))
            else:
                self.total[:, span] = quad_sum

    def run(self, compute):
        count = len(self.spans)
        compute(*self.spans[0])
        self.direct(0)
        for c in range(count):
            if c + 1 < count:
                compute(*self.spans[c + 1])
                self.direct(c + 1)
            self.follow(c)
            if c:
                self.settle(c - 1)
        self.settle(count - 1)
        for c in range(count):
            span = pl.ds(*self.spans[c])
            for k in self.steps[:-1]:
                self.copies[6, k, c].wait_recv()
                self.total[:, span] += self.got_z[k, :, span].astype(F32)
        for copy in self.copies.values():
            copy.wait_send()


def low_of(c, span):
    return pl.ds(c * span.size, span.size)


def attend_row(region, row, query, fresh_keys, fresh_values, position, count, key_heads):
    head_size = query.shape[1]
    group = query.shape[0] // key_heads
    kv_cols = key_heads * head_size
    inv_root = head_size ** (-0.5)
    wide = jnp.concatenate([query] * key_heads, axis=1)
    owner = lax.broadcasted_iota(jnp.int32, wide.shape, 0) // group
    column = lax.broadcasted_iota(jnp.int32, wide.shape, 1) // head_size
    wide = jnp.where(owner == column, wide, 0.0).astype(BF16)
    span = pl.ds(pl.multiple_of(row * count, count), count)
    scores = lax.dot_general(wide, region[span, :kv_cols], NT, preferred_element_type=F32) * inv_root
    fresh = lax.dot_general(wide, fresh_keys, NT, preferred_element_type=F32) * inv_root
    spot = lax.broadcasted_iota(jnp.int32, scores.shape, 1).astype(F32)
    scores = jnp.where(spot < position, scores, -1e30)
    fresh = jnp.where(lax.broadcasted_iota(jnp.int32, fresh.shape, 1) == row, fresh, -1e30)
    peak = jnp.maximum(
        jnp.max(scores, axis=1, keepdims=True), jnp.max(fresh, axis=1, keepdims=True)
    )
    weights = jnp.exp(scores - peak)
    fresh_w = jnp.exp(fresh - peak)
    scale = 1.0 / (
        jnp.sum(weights, axis=1, keepdims=True) + jnp.sum(fresh_w, axis=1, keepdims=True)
    )
    full = jnp.dot(
        (weights * scale).astype(BF16), region[span, kv_cols:], preferred_element_type=F32
    ) + jnp.dot((fresh_w * scale).astype(BF16), fresh_values, preferred_element_type=F32)
    full = jnp.where(owner == column, full, 0.0)
    result = full[:, :head_size]
    for k in range(1, key_heads):
        result = result + full[:, k * head_size : (k + 1) * head_size]
    return result


def layer_kernel(
    lines, names, stream, cache, w_qkv, w_out, w_gate_up, w_down, lm_head,
    table, factors, inner, targets, out, logprob, *refs
):
    s = SimpleNamespace(**dict(zip(names, refs)))
    place = Place(lines)
    tp_count = lines * QUAD
    member = place.member
    other = {"member": 1 - member}
    own_rows, width = s.own.shape
    region, gate_up, block = s.region, s.gate_up, s.block
    count = cache.shape[1]
    ff = w_down.shape[0]
    half = width // 2

    loads = {}

    def load(name, i, src, dst):
        loads[name] = pltpu.make_async_copy(src, dst, s.loads.at[i])
        loads[name].start()

    barrier = pltpu.get_barrier_semaphore()
    others = []
    for core in (member, 1 - member):
        for step in range(tp_count):
            if others or step:
                others.append({"member": core, "tp": lax.rem(place.tp + step, tp_count)})
    for device in others:
        pl.semaphore_signal(barrier, inc=1, device_id=device, device_id_type=pl.DeviceIdType.MESH)
    load("stream", 0, stream, s.stream)
    qkv = gate_up.at[0, :, pl.ds(0, w_qkv.shape[1])]
    load("qkv", 1, w_qkv, qkv)
    for r in range(own_rows):
        load(("row", r), 6 + r, cache.at[r], region.at[pl.ds(r * count, count)])
    load("out", 2, w_out, s.w_out)
    loads["stream"].wait()
    mine = pl.ds(pl.multiple_of(place.tp * own_rows, own_rows), own_rows)
    block[mine, :] = norm_rows(s.stream[...].astype(F32), factors[0:1, :]).astype(BF16)
    pl.semaphore_wait(barrier, len(others))

    piece = width // CHUNKS
    spans = [(c * piece, piece) for c in range(CHUNKS)]
    first_sums = s.acts.at[0, :, pl.ds(0, w_qkv.shape[1])]
    waited = []

    def project(start, size):
        if not waited:
            loads["qkv"].wait()
            waited.append(True)
        span = pl.ds(start, size)
        step = jnp.dot(block[:, span], qkv[span, :], preferred_element_type=F32)
        if start:
            first_sums[...] += step
        else:
            first_sums[...] = step

    Gather(place, block, own_rows, spans, (s.ga_send, s.ga_recv)).run(project)
    s.proj[...] = first_sums[...].astype(BF16)
    load("gate_up", 3, w_gate_up, gate_up)

    def peers(k):
        return lax.rem(place.tp + k, tp_count)

    copies = []
    for k in range(1, tp_count):
        rows = pl.ds(pl.multiple_of(peers(k) * own_rows, own_rows), own_rows)
        copies.append(
            remote(
                s.proj.at[rows], s.rows_in.at[place.tp],
                s.xa_send.at[k], s.xa_recv.at[k], {"tp": peers(k)},
            )
        )
    s.rows_in[place.tp] = s.proj[mine, :]
    for copy in copies:
        copy.wait_recv()
    per_device = s.proj.shape[1] // HD
    cos, sin = table[0], table[1]

    def head(h):
        column = (h % per_device) * HD
        return s.rows_in[h // per_device, :, column : column + HD]

    def turned(h):
        value = head(h).astype(F32)
        return (value * cos + pltpu.roll(value, HD // 2, 1) * sin).astype(BF16)

    for h in range(HEADS):
        s.queries[h * own_rows : (h + 1) * own_rows, :] = turned(h).astype(F32)
    for k in range(KV):
        s.keys[:, k * HD : (k + 1) * HD] = turned(HEADS + k)
        s.values[:, k * HD : (k + 1) * HD] = head(HEADS + KV + k)
    for r in range(own_rows):
        loads["row", r].wait()
    unroll = 4

    @pl.loop(0, own_rows // unroll)
    def _(i):
        for j in range(unroll):
            r = i * unroll + j
            strided = pl.ds(r, HEADS, stride=own_rows)
            s.attended[strided, :] = attend_row(
                region, r, s.queries[strided, :], s.keys[...], s.values[...],
                table[2, pl.ds(r, 1), :][:, :1], count, KV,
            )

    load("down_0", 4, w_down.at[:, pl.ds(0, half)], region.at[pl.ds(width, ff)])
    load("down_1", 5, w_down.at[:, pl.ds(half, half)], region.at[pl.ds(width + ff, ff)])
    cols = lm_head.shape[1] // 2
    load(
        "words", 0, lm_head.at[:, pl.ds(pl.multiple_of(member * cols, cols), cols)],
        region.at[pl.ds(0, width)],
    )
    own_heads = w_out.shape[0] // HD
    for d in range(tp_count):
        for i in range(own_heads):
            h = d * own_heads + i
            s.heads_out[d, :, i * HD : (i + 1) * HD] = s.attended[
                h * own_rows : (h + 1) * own_rows, :
            ].astype(BF16)
    for copy in copies:
        copy.wait_send()
    copies = []
    for k in range(1, tp_count):
        copies.append(
            remote(
                s.heads_out.at[peers(k)], s.heads_in.at[mine],
                s.xb_send.at[k], s.xb_recv.at[k], {"tp": peers(k)},
            )
        )
    s.heads_in[mine, :] = s.heads_out[place.tp]
    loads["out"].wait()
    for copy in copies:
        copy.wait_recv()
    part, total = s.part, s.total
    sums = [s.got_dx, s.got_dy, s.put_x, s.put_y, s.got_x, s.got_y, s.put_z, s.got_z]

    def project_out(start, size):
        span = pl.ds(start, size)
        part[:, span] = jnp.dot(
            s.heads_in[...], s.w_out[:, span], preferred_element_type=F32
        ).astype(BF16)

    Reduce(place, part, total, own_rows, spans, (s.ra_send, s.ra_recv), sums).run(project_out)
    for copy in copies:
        copy.wait_send()
    middle = s.middle
    middle[...] = (s.stream[...].astype(F32) + total[...]).astype(BF16)
    block[mine, :] = norm_rows(middle[...].astype(F32), factors[1:2, :]).astype(BF16)
    members, batch = 2, s.final.shape[1]
    acts, hidden = s.acts, s.hidden
    waited_up = []

    def gate_and_up(start, size):
        if not waited_up:
            loads["gate_up"].wait()
            acts[...] = jnp.zeros_like(acts)
            waited_up.append(True)
        wide = 512

        @pl.loop(0, size // wide)
        def _(i):
            span = pl.ds(pl.multiple_of(start + i * wide, wide), wide)
            values = block[:, span].astype(F32)
            for j in range(2):
                scaled = jnp.concatenate(
                    [
                        values[m * batch : (m + 1) * batch] * factors[3 + 2 * m + j : 4 + 2 * m + j, span]
                        for m in range(members)
                    ],
                    axis=0,
                ).astype(BF16)
                acts[j] += jnp.dot(scaled, gate_up[j, span, :], preferred_element_type=F32)

    Gather(place, block, own_rows, spans, (s.gb_send, s.gb_recv)).run(gate_and_up)
    for m in range(members):
        rows = slice(m * batch, (m + 1) * batch)
        gate = acts[0, rows, :] * inner[3 * m : 3 * m + 1, :]
        hidden[rows, :] = (
            gate / (1.0 + jnp.exp(-gate))
            * (acts[1, rows, :] * inner[3 * m + 1 : 3 * m + 2, :])
            * inner[3 * m + 2 : 3 * m + 3, :]
        ).astype(BF16)
    loads["down_0"].wait()
    loads["down_1"].wait()

    def project_down(start, size):
        side = start // half
        rows = pl.ds(width + side * ff, ff)
        part[:, pl.ds(start, size)] = jnp.dot(
            hidden[...], region[rows, pl.ds(start - side * half, size)],
            preferred_element_type=F32,
        ).astype(BF16)

    Reduce(place, part, total, own_rows, spans, (s.rb_send, s.rb_recv), sums).run(project_down)
    own_member = place.tp * own_rows // batch
    scale = jnp.where(own_member == 0, factors[7:8, :], factors[8:9, :])
    layer_out = (middle[...].astype(F32) + total[...] * scale).astype(BF16)
    s.own[...] = norm_rows(layer_out.astype(F32), factors[2:3, :]).astype(BF16)
    first = member == 0
    low, high = s.own[:, :half].astype(F32), s.own[:, half:].astype(F32)
    half_own, pair = s.half_own, s.pair
    half_own[...] = jnp.where(first, low, high)
    s.away[...] = jnp.where(first, high, low).astype(BF16)
    core = remote(s.away, s.from_core, s.side_send.at[0], s.side_recv.at[0], other)
    core.wait_recv()
    half_own[...] = half_own[...] + s.from_core[...].astype(F32)
    pair[...] = half_own[...]
    twin = remote(
        pair, s.from_pair, s.side_send.at[1], s.side_recv.at[1], place.to_line(lines // 2)
    )
    twin.wait_recv()
    turn = 1 - 2 * lax.rem(place.line, 2)

    class Pairwise:
        lines = 2
        quad, quad_x, quad_y = place.quad, place.quad_x, place.quad_y
        to_x, to_y = place.to_x, place.to_y

        @staticmethod
        def line_at(step):
            return lax.rem(place.line + abs(step), 2)

        @staticmethod
        def to_line(step):
            return {"tp": (place.line + turn) * QUAD + place.quad}

    final = s.final
    at = lax.rem(place.line, 2) * QUAD + place.quad
    final[member, pl.ds(pl.multiple_of(at * own_rows, own_rows), own_rows), :] = (
        (half_own[...] + s.from_pair[...]) * 0.25
    ).astype(BF16)
    words = region.at[pl.ds(0, width)]
    shares = []

    def share(start, size):
        view = final.at[member, :, pl.ds(start, size)]
        shares.append(
            remote(
                view, view, s.share_send.at[len(shares)], s.share_recv.at[len(shares)], other
            )
        )

    last = half // 2
    Gather(
        Pairwise, final.at[member], own_rows, [(0, last), (last, last)], (s.gc_send, s.gc_recv)
    ).run(share)
    loads["words"].wait()
    for copy in shares:
        copy.wait_recv()
    tile_count = s.tile_send.shape[0]
    tile_width = cols // tile_count
    column = lax.broadcasted_iota(jnp.int32, (batch, batch), 1)
    corner = lax.broadcasted_iota(jnp.int32, (batch, batch), 0) == column
    wanted = jnp.sum(
        jnp.where(corner, targets[...].astype(F32), 0.0), axis=-1, keepdims=True
    ).astype(jnp.int32)
    peak = jnp.full((batch, 1), -jnp.inf, F32)
    amount = jnp.zeros((batch, 1), F32)
    found = jnp.zeros((batch, 1), F32)
    tiles = []
    for i in range(tile_count):
        span = pl.ds(i * tile_width, tile_width)
        tile = jnp.dot(final[0], words[:half, span], preferred_element_type=F32) + jnp.dot(
            final[1], words[half:, span], preferred_element_type=F32
        )
        into = out.at[:, pl.ds(pl.multiple_of(member * cols + i * tile_width, tile_width), tile_width)]
        into[...] = tile.astype(BF16)
        tiles.append(remote(into, into, s.tile_send.at[i], s.tile_recv.at[i], other))
        new = jnp.maximum(peak, jnp.max(tile, axis=-1, keepdims=True))
        amount = amount * jnp.exp(peak - new) + jnp.sum(
            jnp.exp(tile - new), axis=-1, keepdims=True
        )
        peak = new
        column = (
            (place.tp * 2 + member) * cols
            + i * tile_width
            + lax.broadcasted_iota(jnp.int32, tile.shape, 1)
        )
        found = found + jnp.sum(jnp.where(column == wanted, tile, 0.0), axis=-1, keepdims=True)
    lane = lax.broadcasted_iota(jnp.int32, (batch, 128), 1)
    facts = jnp.where(lane == 0, peak, jnp.where(lane == 1, amount, found))
    stats, board = s.stats, s.board
    stats[...] = jnp.transpose(facts)[:8, :]
    copies = []
    for slot, device in enumerate(others):
        copies.append(
            remote(
                stats, board.at[slot + 1], s.stat_send.at[slot], s.stat_recv.at[slot], device
            )
        )
    board[0] = stats[...]
    for copy in copies:
        copy.wait_recv()
    top = jnp.max(board[:, 0, :], axis=0, keepdims=True)
    amount = jnp.sum(board[:, 1, :] * jnp.exp(board[:, 0, :] - top), axis=0, keepdims=True)
    found = jnp.sum(board[:, 2, :], axis=0, keepdims=True)
    logprob[...] = found - (top + jnp.log(amount))
    for copy in tiles:
        copy.wait_recv()
    for copy in [core, twin] + shares + tiles + copies:
        copy.wait_send()


VMEM = pl.BlockSpec(memory_space=pltpu.VMEM)
ANY = pl.BlockSpec(memory_space=pl.ANY)


def fused_body(
    stream_in,
    kv_cache,
    lengths,
    targets,
    norm_gains,
    w_qkv,
    w_out,
    w_gate_up,
    w_down,
    lm_head,
    fast_in,
    fast_hidden,
    fast_out,
):
    tp_count = lax.axis_size("tp")
    tp_rank = lax.axis_index("tp")
    lines = tp_count // QUAD
    batch = lengths.shape[0]
    own_rows, width = stream_in.shape
    all_rows = own_rows * tp_count
    half = width // 2
    devices = 2 * tp_count
    vocab_cols = lm_head.shape[1]
    ff = w_down.shape[0]
    positions = lax.dynamic_slice_in_dim(
        lengths, (tp_rank * own_rows) % batch, own_rows, 0
    ).astype(F32)
    frequency = ROPE_BASE ** (-jnp.arange(HD // 2, dtype=F32) * 2.0 / HD)
    angles = positions[:, None] * frequency[None, :]
    cos, sin = jnp.cos(angles), jnp.sin(angles)
    table = jnp.stack(
        [
            jnp.concatenate([cos, cos], axis=1),
            jnp.concatenate([-sin, sin], axis=1),
            jnp.broadcast_to(positions[:, None], (own_rows, HD)),
        ]
    )
    factors = jnp.concatenate(
        [norm_gains, fast_in.reshape(4, width), fast_out, jnp.zeros((7, width), F32)]
    )
    inner = jnp.concatenate([fast_hidden.reshape(6, ff), jnp.zeros((10, ff), F32)])
    tiles = 4
    small = pltpu.VMEM((lines, own_rows, half), BF16)
    large = pltpu.VMEM((lines, own_rows, width), BF16)
    own = pltpu.VMEM((own_rows, width), BF16)
    gather = DMA((5, lines, CHUNKS))
    reduce = DMA((7, lines, CHUNKS))
    scratch = dict(
        region=pltpu.VMEM((own_rows * kv_cache.shape[1], kv_cache.shape[2]), BF16),
        gate_up=pltpu.VMEM(w_gate_up.shape, BF16),
        w_out=pltpu.VMEM(w_out.shape, BF16),
        block=pltpu.VMEM((all_rows, width), BF16),
        part=pltpu.VMEM((all_rows, width), BF16),
        stream=own,
        own=own,
        middle=own,
        total=pltpu.VMEM((own_rows, width), F32),
        proj=pltpu.VMEM((all_rows, w_qkv.shape[1]), BF16),
        rows_in=pltpu.VMEM((tp_count, own_rows, w_qkv.shape[1]), BF16),
        queries=pltpu.VMEM(((HEADS + 1) * own_rows, HD), F32),
        keys=pltpu.VMEM((own_rows, KV * HD), BF16),
        values=pltpu.VMEM((own_rows, KV * HD), BF16),
        attended=pltpu.VMEM(((HEADS + 1) * own_rows, HD), F32),
        heads_out=pltpu.VMEM((tp_count, own_rows, w_out.shape[0]), BF16),
        heads_in=pltpu.VMEM((all_rows, w_out.shape[0]), BF16),
        acts=pltpu.VMEM((2, all_rows, ff), F32),
        hidden=pltpu.VMEM((all_rows, ff), BF16),
        half_own=pltpu.VMEM((own_rows, half), F32),
        away=pltpu.VMEM((own_rows, half), BF16),
        from_core=pltpu.VMEM((own_rows, half), BF16),
        pair=pltpu.VMEM((own_rows, half), F32),
        from_pair=pltpu.VMEM((own_rows, half), F32),
        final=pltpu.VMEM((2, batch, half), BF16),
        stats=pltpu.VMEM((8, batch), F32),
        board=pltpu.VMEM((devices, 8, batch), F32),
        got_dx=small, got_dy=small, put_x=small, put_y=small,
        got_x=large, got_y=large, put_z=large, got_z=large,
        loads=DMA((6 + own_rows,)),
        ga_send=gather, ga_recv=gather, gb_send=gather, gb_recv=gather,
        ra_send=reduce, ra_recv=reduce, rb_send=reduce, rb_recv=reduce,
        gc_send=DMA((5, 2, 2)), gc_recv=DMA((5, 2, 2)),
        xa_send=DMA((tp_count,)), xa_recv=DMA((tp_count,)),
        xb_send=DMA((tp_count,)), xb_recv=DMA((tp_count,)),
        side_send=DMA((2,)), side_recv=DMA((2,)),
        share_send=DMA((2,)), share_recv=DMA((2,)),
        tile_send=DMA((tiles,)), tile_recv=DMA((tiles,)),
        stat_send=DMA((devices,)), stat_recv=DMA((devices,)),
    )
    mean_logits, logprob = pl.pallas_call(
        functools.partial(layer_kernel, lines, tuple(scratch)),
        out_shape=[
            jax.ShapeDtypeStruct((batch, vocab_cols), BF16),
            jax.ShapeDtypeStruct((1, batch), F32),
        ],
        in_specs=[ANY] * 7 + [VMEM] * 4,
        out_specs=[VMEM, VMEM],
        scratch_shapes=list(scratch.values()),
        compiler_params=pltpu.CompilerParams(
            collective_id=1, has_side_effects=True, vmem_limit_bytes=VMEM_BYTES
        ),
    )(
        stream_in, kv_cache, w_qkv, w_out, w_gate_up, w_down, lm_head,
        table, factors, inner, targets[None, :],
    )
    return (mean_logits, logprob[0])


VMEM_BYTES = 67043328


def body(*args):
    stream_in, kv_cache, lengths = args[0], args[1], args[2]
    w_qkv, w_out, w_down, lm_head, fast_in = args[5], args[6], args[8], args[9], args[10]
    own_rows, width = stream_in.shape
    batch, ff = lengths.shape[0], w_down.shape[0]
    tp_count = lax.axis_size("tp")
    fits = (
        tp_count == 4 * QUAD
        and own_rows == 16
        and batch == 128
        and lax.axis_size("member") == 2
        and fast_in.shape[0] == 2
        and own_rows * tp_count == 2 * batch
        and w_qkv.shape[1] % HD == 0
        and w_out.shape[0] % HD == 0
        and w_qkv.shape[1] <= ff
        and width % (256 * CHUNKS) == 0
        and kv_cache.shape[2] * 2 == width
        and lm_head.shape[1] == width
        and own_rows * kv_cache.shape[1] >= width + 2 * ff
    )
    if fits:
        return fused_body(*args)
    return plain_body(*args)


def solution(mesh):
    in_specs = (
        P(("member", "tp"), None),
        P(("member", "tp"), None, None),
        P(),
        P(),
        P(),
        P(None, "tp"),
        P("tp", None),
        P(None, None, "tp"),
        P("tp", None),
        P(None, "tp"),
        P("member", None, None),
        P("member", None, "tp"),
        P("member", None),
    )
    out_specs = (P(None, "tp"), P())
    return jax.shard_map(body, mesh=mesh, in_specs=in_specs, out_specs=out_specs, check_vma=False)
```

```python
import functools
from types import SimpleNamespace

import jax
import jax.numpy as jnp
from jax import lax
from jax.experimental import pallas as pl
from jax.experimental.pallas import tpu as pltpu
from jax.sharding import PartitionSpec as P

HEADS = 32
KV = 8
HD = 128
CACHE = 512


ROPE_BASE = 500000.0


def rms_norm(values_in, gain):
    return (
        values_in
        * lax.rsqrt(jnp.mean(values_in * values_in, axis=-1, keepdims=True) + 1e-05)
        * gain
    )


def rotate(values_in, positions):
    half_dim = values_in.shape[-1] // 2
    frequency = ROPE_BASE ** (-jnp.arange(half_dim, dtype=jnp.float32) * 2.0 / values_in.shape[-1])
    angles = positions.astype(jnp.float32)[:, None, None] * frequency[None, None, :]
    lower_half = values_in[..., :half_dim]
    upper_half = values_in[..., half_dim:]
    return jnp.concatenate(
        [
            lower_half * jnp.cos(angles) - upper_half * jnp.sin(angles),
            upper_half * jnp.cos(angles) + lower_half * jnp.sin(angles),
        ],
        axis=-1,
    )


def attend(projected, cache_rows, positions):
    row_count = projected.shape[0]
    head_cols = HEADS * HD
    kv_cols = KV * HD
    queries = rotate(
        projected[:, :head_cols].astype(jnp.float32).reshape(row_count, HEADS, HD), positions
    ).astype(jnp.bfloat16)
    new_key = rotate(
        projected[:, head_cols : head_cols + kv_cols]
        .astype(jnp.float32)
        .reshape(row_count, KV, HD),
        positions,
    ).astype(jnp.bfloat16)
    new_value = projected[:, head_cols + kv_cols :].reshape(row_count, KV, HD)
    cache_keys = cache_rows[:, :, :kv_cols].reshape(row_count, CACHE, KV, HD)
    cache_values = cache_rows[:, :, kv_cols:].reshape(row_count, CACHE, KV, HD)
    grouped = queries.reshape(row_count, KV, HEADS // KV, HD)
    inv_root = HD ** (-0.5)
    cached = (
        jnp.einsum("rkgd,rckd->rkgc", grouped, cache_keys, preferred_element_type=jnp.float32)
        * inv_root
    )
    fresh = (
        jnp.einsum("rkgd,rkd->rkg", grouped, new_key, preferred_element_type=jnp.float32) * inv_root
    )
    in_cache = jnp.arange(CACHE)[None, :] < positions[:, None]
    cached = jnp.where(in_cache[:, None, None, :], cached, -1e30)
    peak = jnp.maximum(jnp.max(cached, axis=-1), fresh)
    weights = jnp.exp(cached - peak[..., None])
    fresh_w = jnp.exp(fresh - peak)
    total_sum = jnp.sum(weights, axis=-1) + fresh_w
    probs = (weights / total_sum[..., None]).astype(jnp.bfloat16)
    fresh_p = (fresh_w / total_sum).astype(jnp.bfloat16)
    result = jnp.einsum("rkgc,rckd->rkgd", probs, cache_values, preferred_element_type=jnp.float32)
    result = (
        result
        + fresh_p.astype(jnp.float32)[..., None] * new_value.astype(jnp.float32)[:, :, None, :]
    )
    return result.reshape(row_count, HEADS * HD).astype(jnp.bfloat16)


def plain_body(
    stream_in,
    kv_cache,
    lengths,
    targets,
    norm_gains,
    w_qkv,
    w_out,
    w_gate_up,
    w_down,
    lm_head,
    fast_in,
    fast_hidden,
    fast_out,
):
    tp_count = lax.axis_size("tp")
    tp_rank = lax.axis_index("tp")
    mem_dev = fast_in.shape[0]
    batch_rows = lengths.shape[0]
    own_rows = stream_in.shape[0]
    all_rows = own_rows * tp_count
    width = stream_in.shape[1]
    first_row = tp_rank * own_rows
    positions = lax.dynamic_slice_in_dim(lengths, first_row % batch_rows, own_rows, 0)
    own_member = first_row // batch_rows
    own_scale = lax.dynamic_index_in_dim(fast_out, own_member, 0, keepdims=True)
    own_normed = rms_norm(stream_in.astype(jnp.float32), norm_gains[0]).astype(jnp.bfloat16)
    attn_in = lax.all_gather(own_normed, "tp", axis=0, tiled=True)
    projected = jnp.dot(attn_in, w_qkv, preferred_element_type=jnp.float32).astype(jnp.bfloat16)
    row_major = lax.all_to_all(projected, "tp", split_axis=0, concat_axis=1, tiled=True)
    attended = attend(row_major, kv_cache, positions)
    head_major = lax.all_to_all(attended, "tp", split_axis=1, concat_axis=0, tiled=True)
    picked = head_major
    attn_sum = lax.psum_scatter(
        jnp.dot(picked, w_out, preferred_element_type=jnp.float32),
        "tp",
        scatter_dimension=0,
        tiled=True,
    )
    middle = (stream_in.astype(jnp.float32) + attn_sum).astype(jnp.bfloat16)
    own_ffn = rms_norm(middle.astype(jnp.float32), norm_gains[1]).astype(jnp.bfloat16)
    ffn_in = lax.all_gather(own_ffn, "tp", axis=0, tiled=True)
    grouped = ffn_in.astype(jnp.float32).reshape(mem_dev, batch_rows, width)
    gate_in = (grouped * fast_in[:, 0][:, None, :]).astype(jnp.bfloat16).reshape(all_rows, width)
    up_in = (grouped * fast_in[:, 1][:, None, :]).astype(jnp.bfloat16).reshape(all_rows, width)
    hidden_cols = w_gate_up.shape[2]
    gate_act = (
        jnp.dot(gate_in, w_gate_up[0], preferred_element_type=jnp.float32).reshape(
            mem_dev, batch_rows, hidden_cols
        )
        * fast_hidden[:, 0][:, None, :]
    )
    up_act = (
        jnp.dot(up_in, w_gate_up[1], preferred_element_type=jnp.float32).reshape(
            mem_dev, batch_rows, hidden_cols
        )
        * fast_hidden[:, 1][:, None, :]
    )
    hidden = (
        (jax.nn.silu(gate_act) * up_act * fast_hidden[:, 2][:, None, :])
        .astype(jnp.bfloat16)
        .reshape(all_rows, hidden_cols)
    )
    picked = hidden
    down_sum = lax.psum_scatter(
        jnp.dot(picked, w_down, preferred_element_type=jnp.float32),
        "tp",
        scatter_dimension=0,
        tiled=True,
    )
    layer_out = (middle.astype(jnp.float32) + down_sum * own_scale).astype(jnp.bfloat16)
    own_final = rms_norm(layer_out.astype(jnp.float32), norm_gains[2]).astype(jnp.bfloat16)
    final_in = lax.all_gather(own_final, "tp", axis=0, tiled=True)
    logits = jnp.dot(final_in, lm_head, preferred_element_type=jnp.float32)
    vocab_cols = lm_head.shape[1]
    member_total = jnp.sum(logits.reshape(mem_dev, batch_rows, vocab_cols), axis=0)
    member_count = mem_dev * lax.axis_size("member")
    mean_logit = (
        lax.psum(member_total.astype(jnp.bfloat16), "member").astype(jnp.float32) / member_count
    )
    column_ids = tp_rank * vocab_cols + jnp.arange(vocab_cols)
    target_part = jnp.sum(
        jnp.where(column_ids[None, :] == targets[:, None], mean_logit, 0.0), axis=-1
    )
    local_peak = jnp.max(mean_logit, axis=-1)
    peak = lax.pmax(local_peak, "tp")
    exp_total, target_logit = lax.psum(
        (jnp.sum(jnp.exp(mean_logit - peak[:, None]), axis=-1), target_part), "tp"
    )
    token_logprob = target_logit - (peak + jnp.log(exp_total))
    return (mean_logit.astype(jnp.bfloat16), token_logprob)


BF16 = jnp.bfloat16
F32 = jnp.float32
DMA = pltpu.SemaphoreType.DMA
QUAD = 4


def norm_rows(values_in, gain):
    return (
        values_in
        * lax.rsqrt(jnp.mean(values_in * values_in, axis=-1, keepdims=True) + 1e-05)
        * gain
    )


class Place:
    def __init__(self, lines):
        self.tp = lax.axis_index("tp")
        self.member = lax.axis_index("member")
        self.lines = lines
        self.quad = lax.rem(self.tp, QUAD)
        self.line = self.tp // QUAD
        self.quad_x = self.quad + 1 - 2 * lax.rem(self.quad, 2)
        self.quad_y = lax.rem(self.quad + 2, QUAD)
        self.quad_d = self.quad_x + self.quad_y - self.quad
        self.to_x = {"tp": self.line * QUAD + self.quad_x}
        self.to_y = {"tp": self.line * QUAD + self.quad_y}
        self.inner = jnp.logical_or(self.line == 1, self.line == 2)
        beside, across, over = (
            self.line + 1 - 2 * lax.rem(self.line, 2),
            lines - 1 - self.line,
            lax.rem(self.line + 2, lines),
        )
        self.near = [
            self.line,
            beside,
            jnp.where(self.inner, across, over),
            jnp.where(self.inner, over, across),
        ]
        self.pair = {"tp": beside * QUAD + self.quad}
        self.middle = {"tp": across * QUAD + self.quad}

    def line_at(self, step):
        return lax.rem(self.line + step + self.lines, self.lines)

    def to_line(self, step):
        return {"tp": self.line_at(step) * QUAD + self.quad}


def remote(src, dst, send_sem, recv_sem, device):
    copy = pltpu.make_async_remote_copy(
        src_ref=src,
        dst_ref=dst,
        send_sem=send_sem,
        recv_sem=recv_sem,
        device_id=device,
        device_id_type=pl.DeviceIdType.MESH,
    )
    copy.start()
    return copy


NT = (((1,), (1,)), ((), ()))
CHUNKS = 2
WORD_LOADS = 8


class PairGather:
    def __init__(self, place, buf, rows, spans, sems):
        self.place, self.buf, self.rows, self.spans = place, buf, rows, spans
        self.sends, self.recvs = sems
        self.copies = {}

    def at(self, step, quad, start, width):
        index = self.place.line_at(step) * QUAD + quad
        rows = pl.ds(pl.multiple_of(index * self.rows, self.rows), self.rows)
        return self.buf.at[rows, pl.ds(start, width)]

    def send(self, kind, k, c, block, device):
        self.copies[kind, k, c] = remote(
            block, block, self.sends.at[kind, k, c], self.recvs.at[kind, k, c], device
        )

    def start(self):
        place = self.place
        for c, (start, width) in enumerate(self.spans):
            mine = self.at(0, place.quad, start, width)
            for k in range(1, place.lines):
                self.send(0, k, c, mine, place.to_line(k))
            self.send(1, 0, c, mine, place.to_x)
            self.send(2, 0, c, mine, place.to_y)

    def spread(self, c):
        place = self.place
        for k in range(1, place.lines):
            self.copies[0, k, c].wait_recv()
            block = self.at(-k, place.quad, *self.spans[c])
            self.send(1, k, c, block, place.to_x)
            self.send(2, k, c, block, place.to_y)
            self.feed()

    def relay(self, c):
        place = self.place
        start, width = self.spans[c]
        half = width // 2
        for k in range(place.lines):
            self.copies[1, k, c].wait_recv()
            self.send(3, k, c, self.at(-k, place.quad_x, start, half), place.to_y)
            self.copies[2, k, c].wait_recv()
            self.send(4, k, c, self.at(-k, place.quad_y, start + half, half), place.to_x)
            self.feed()

    def arrive(self, c):
        for k in range(self.place.lines):
            self.copies[3, k, c].wait_recv()
            self.copies[4, k, c].wait_recv()

    def run(self, compute, feed=lambda: None):
        count = len(self.spans)
        self.feed = feed
        self.start()
        self.spread(0)
        for c in range(count):
            if c + 1 < count:
                self.spread(c + 1)
            self.relay(c)
            if c:
                self.arrive(c - 1)
                compute(*self.spans[c - 1])
        self.arrive(count - 1)
        compute(*self.spans[count - 1])
        for copy in self.copies.values():
            copy.wait_send()


class Gather:
    def __init__(self, place, buf, rows, spans, side, sems):
        self.place, self.buf, self.rows = place, buf, rows
        self.spans, self.side = spans, side
        self.sends, self.recvs = sems
        self.copies, self.guarded = {}, []

    def at(self, line, quad, start, width):
        index = line * QUAD + quad
        rows = pl.ds(pl.multiple_of(index * self.rows, self.rows), self.rows)
        return self.buf.at[rows, pl.ds(start, width)]

    def plane(self, line, start, width):
        rows = QUAD * self.rows
        return self.buf.at[pl.ds(pl.multiple_of(line * rows, rows), rows), pl.ds(start, width)]

    def send(self, kind, k, c, block, device):
        self.copies[kind, k, c] = remote(
            block, block, self.sends.at[kind, k, c], self.recvs.at[kind, k, c], device
        )

    def cross(self, slot, k, c, block, device, inner):
        copy = pltpu.make_async_remote_copy(
            src_ref=block, dst_ref=block,
            send_sem=self.sends.at[slot, k, c], recv_sem=self.recvs.at[0, slot_of(slot, k), c],
            device_id=device, device_id_type=pl.DeviceIdType.MESH,
        )
        if inner:
            self.guarded.append(copy)

            @pl.when(self.place.inner)
            def _():
                copy.start()
        else:
            copy.start()
            self.copies[slot, k, c] = copy

    def await_line(self, k, c, block):
        pltpu.make_async_remote_copy(
            src_ref=block, dst_ref=block,
            send_sem=self.sends.at[0, k, c], recv_sem=self.recvs.at[0, k, c],
            device_id=self.place.pair, device_id_type=pl.DeviceIdType.MESH,
        ).wait_recv()

    def own_line(self, c, block):
        self.cross(5, 0, c, block, self.place.pair, False)
        self.cross(6, 0, c, block, self.place.middle, True)

    def pass_line(self, k, c, block):
        if k == 1:
            self.cross(6, 1, c, block, self.place.middle, True)
        else:
            self.cross(5, k - 1, c, block, self.place.pair, True)

    def start(self):
        place = self.place
        count = len(self.spans)
        for c, span in enumerate(self.spans):
            self.own_line(c, self.at(place.line, place.quad, *span))
        for c, span in [(count, self.side)] + list(enumerate(self.spans)):
            mine = self.at(place.line, place.quad, *span)
            self.send(1, 0, c, mine, place.to_x)
            self.send(2, 0, c, mine, place.to_y)

    def spread(self, c):
        place = self.place
        for k in range(1, place.lines):
            block = self.at(place.near[k], place.quad, *self.spans[c])
            self.await_line(k, c, block)
            self.pass_line(k, c, block)
            self.send(1, k, c, block, place.to_x)
            self.send(2, k, c, block, place.to_y)
            self.feed()

    def relay(self, c, k):
        place = self.place
        start, width = (self.spans + [self.side])[c]
        half = width // 256 * 128
        self.copies[1, k, c].wait_recv()
        self.send(3, k, c, self.at(place.near[k], place.quad_x, start, half), place.to_y)
        self.copies[2, k, c].wait_recv()
        self.send(
            4, k, c, self.at(place.near[k], place.quad_y, start + half, width - half), place.to_x
        )

    def arrive(self, c):
        for k in range(self.place.lines):
            self.copies[3, k, c].wait_recv()
            self.copies[4, k, c].wait_recv()

    def side_step(self, k):
        c = len(self.spans)
        if k == 0:
            self.copies[3, 0, c].wait_recv()
            self.copies[4, 0, c].wait_recv()
            self.own_line(c, self.plane(self.place.line, *self.side))
        else:
            block = self.plane(self.place.near[k], *self.side)
            self.await_line(k, c, block)
            self.pass_line(k, c, block)

    def run(self, compute, feed=lambda: None):
        place = self.place
        count = len(self.spans)
        self.feed = feed
        self.start()
        self.relay(count, 0)
        self.spread(0)
        self.side_step(0)
        for c in range(count):
            if c + 1 < count:
                self.spread(c + 1)
            if c:
                self.side_step(c)
            for k in range(place.lines):
                self.relay(c, k)
                self.feed()
            if c:
                self.arrive(c - 1)
                compute(*self.spans[c - 1])
        for k in range(count, place.lines):
            self.side_step(k)
        compute(*self.side)
        self.arrive(count - 1)
        compute(*self.spans[count - 1])
        for copy in self.copies.values():
            copy.wait_send()

        @pl.when(place.inner)
        def _():
            for copy in self.guarded:
                copy.wait_send()


def slot_of(slot, k):
    if slot == 5:
        return k + 1
    return k + 2


class Reduce:
    def __init__(self, place, part, total, rows, spans, sems, bufs):
        self.place, self.part, self.total = place, part, total
        self.rows, self.spans = rows, spans
        self.sends, self.recvs = sems
        self.got_dx, self.got_dy, self.put_x, self.put_y = bufs[:4]
        self.got_x, self.got_y, self.put_z, self.got_z = bufs[4:]
        self.steps = list(range(1, place.lines)) + [0]
        self.copies = {}

    def at(self, step, quad):
        index = self.place.line_at(step) * QUAD + quad
        return pl.ds(pl.multiple_of(index * self.rows, self.rows), self.rows)

    def send(self, kind, k, c, src, dst, device):
        self.copies[kind, k, c] = remote(
            src, dst, self.sends.at[kind, k, c], self.recvs.at[kind, k, c], device
        )

    def halves(self, c):
        start, width = self.spans[c]
        return pl.ds(start, width // 2), pl.ds(start + width // 2, width // 2)

    def direct(self, c):
        place, part = self.place, self.part
        low, high = self.halves(c)
        for k in self.steps:
            diag = self.at(k, place.quad_d)
            self.send(0, k, c, part.at[diag, high], self.got_dx.at[k, :, low_of(c, high)], place.to_x)
            self.send(1, k, c, part.at[diag, low], self.got_dy.at[k, :, low_of(c, low)], place.to_y)
        for k in self.steps:
            self.send(2, k, c, part.at[self.at(k, place.quad_x), high], self.got_x.at[k, :, high], place.to_x)
            self.send(3, k, c, part.at[self.at(k, place.quad_y), low], self.got_y.at[k, :, low], place.to_y)

    def follow(self, c):
        place, part = self.place, self.part
        low, high = self.halves(c)
        packed = low_of(c, low)
        for k in self.steps:
            self.copies[1, k, c].wait_recv()
            self.put_x[k, :, packed] = (
                part[self.at(k, place.quad_x), low].astype(F32)
                + self.got_dy[k, :, packed].astype(F32)
            ).astype(BF16)
            self.send(4, k, c, self.put_x.at[k, :, packed], self.got_x.at[k, :, low], place.to_x)
            self.copies[0, k, c].wait_recv()
            self.put_y[k, :, packed] = (
                part[self.at(k, place.quad_y), high].astype(F32)
                + self.got_dx[k, :, packed].astype(F32)
            ).astype(BF16)
            self.send(5, k, c, self.put_y.at[k, :, packed], self.got_y.at[k, :, high], place.to_y)
            self.feed()

    def settle(self, c):
        place, part = self.place, self.part
        span = pl.ds(*self.spans[c])
        for k in self.steps:
            for kind in (2, 3, 4, 5):
                self.copies[kind, k, c].wait_recv()
            quad_sum = (
                part[self.at(k, place.quad), span].astype(F32)
                + self.got_x[k, :, span].astype(F32)
                + self.got_y[k, :, span].astype(F32)
            )
            if k:
                self.put_z[k, :, span] = quad_sum.astype(BF16)
                self.send(6, k, c, self.put_z.at[k, :, span], self.got_z.at[k, :, span], place.to_line(k))
            else:
                self.total[:, span] = quad_sum
            self.feed()

    def run(self, compute, feed=lambda: None):
        count = len(self.spans)
        self.feed = feed
        compute(*self.spans[0])
        self.direct(0)
        for c in range(count):
            if c + 1 < count:
                compute(*self.spans[c + 1])
                self.direct(c + 1)
            self.follow(c)
            if c:
                self.settle(c - 1)
        self.settle(count - 1)
        for c in range(count):
            span = pl.ds(*self.spans[c])
            for k in self.steps[:-1]:
                self.copies[6, k, c].wait_recv()
                self.total[:, span] += self.got_z[k, :, span].astype(F32)
        for copy in self.copies.values():
            copy.wait_send()


def low_of(c, span):
    return pl.ds(c * span.size, span.size)


def attend_row(region, row, query, fresh_keys, fresh_values, position, count, key_heads):
    head_size = query.shape[1]
    group = query.shape[0] // key_heads
    kv_cols = key_heads * head_size
    inv_root = head_size ** (-0.5)
    wide = jnp.concatenate([query] * key_heads, axis=1)
    owner = lax.broadcasted_iota(jnp.int32, wide.shape, 0) // group
    column = lax.broadcasted_iota(jnp.int32, wide.shape, 1) // head_size
    wide = jnp.where(owner == column, wide, 0.0).astype(BF16)
    span = pl.ds(pl.multiple_of(row * count, count), count)
    scores = lax.dot_general(wide, region[span, :kv_cols], NT, preferred_element_type=F32) * inv_root
    fresh = lax.dot_general(wide, fresh_keys, NT, preferred_element_type=F32) * inv_root
    spot = lax.broadcasted_iota(jnp.int32, scores.shape, 1).astype(F32)
    scores = jnp.where(spot < position, scores, -1e30)
    fresh = jnp.where(lax.broadcasted_iota(jnp.int32, fresh.shape, 1) == row, fresh, -1e30)
    peak = jnp.maximum(
        jnp.max(scores, axis=1, keepdims=True), jnp.max(fresh, axis=1, keepdims=True)
    )
    weights = jnp.exp(scores - peak)
    fresh_w = jnp.exp(fresh - peak)
    scale = 1.0 / (
        jnp.sum(weights, axis=1, keepdims=True) + jnp.sum(fresh_w, axis=1, keepdims=True)
    )
    full = jnp.dot(
        (weights * scale).astype(BF16), region[span, kv_cols:], preferred_element_type=F32
    ) + jnp.dot((fresh_w * scale).astype(BF16), fresh_values, preferred_element_type=F32)
    full = jnp.where(owner == column, full, 0.0)
    result = full[:, :head_size]
    for k in range(1, key_heads):
        result = result + full[:, k * head_size : (k + 1) * head_size]
    return result


def layer_kernel(
    lines, names, stream, cache, w_qkv, w_out, w_gate_up, w_down, lm_head,
    table, gains, fast_in, fast_hidden, fast_out, targets, out, logprob, *refs
):
    s = SimpleNamespace(**dict(zip(names, refs)))
    place = Place(lines)
    tp_count = lines * QUAD
    member = place.member
    other = {"member": 1 - member}
    own_rows, width = s.own.shape
    region, gate_up, block = s.region, s.gate_up, s.block
    count = cache.shape[1]
    ff = w_down.shape[0]
    half = width // 2

    loads = {}

    def load(name, i, src, dst):
        loads[name] = pltpu.make_async_copy(src, dst, s.loads.at[i])
        loads[name].start()

    barrier = pltpu.get_barrier_semaphore()
    others = []
    for core in (member, 1 - member):
        for step in range(tp_count):
            if others or step:
                others.append({"member": core, "tp": lax.rem(place.tp + step, tp_count)})
    for device in others:
        pl.semaphore_signal(barrier, inc=1, device_id=device, device_id_type=pl.DeviceIdType.MESH)
    load("stream", 0, stream, s.stream)
    qkv = gate_up.at[0, :, pl.ds(0, w_qkv.shape[1])]
    load("qkv", 1, w_qkv, qkv)
    waiting = [
        functools.partial(load, ("row", r), 6 + r, cache.at[r], region.at[pl.ds(r * count, count)])
        for r in range(own_rows)
    ]
    waiting.append(functools.partial(load, "out", 2, w_out, s.w_out))

    def feed():
        if waiting:
            waiting.pop(0)()

    loads["stream"].wait()
    mine = pl.ds(pl.multiple_of(place.tp * own_rows, own_rows), own_rows)
    block[mine, :] = norm_rows(s.stream[...].astype(F32), gains[...][0:1]).astype(BF16)
    pl.semaphore_wait(barrier, len(others))

    piece = width // CHUNKS
    spans = [(c * piece, piece) for c in range(CHUNKS)]
    eighth, last = width // 8, width * 5 // 16
    parts = [(0, width - eighth - last), (width - eighth - last, last)]
    side = (width - eighth, eighth)
    first_sums = s.acts.at[0, :, pl.ds(0, w_qkv.shape[1])]
    waited = []

    def project(start, size):
        if not waited:
            loads["qkv"].wait()
            waited.append(True)
        span = pl.ds(start, size)
        step = jnp.dot(block[:, span], qkv[span, :], preferred_element_type=F32)
        if start:
            first_sums[...] += step
        else:
            first_sums[...] = step

    Gather(place, block, own_rows, parts, side, (s.ga_send, s.ga_recv)).run(project, feed)
    while waiting:
        feed()
    s.proj[...] = first_sums[...].astype(BF16)

    def peers(k):
        return lax.rem(place.tp + k, tp_count)

    copies = []
    for k in range(1, tp_count):
        rows = pl.ds(pl.multiple_of(peers(k) * own_rows, own_rows), own_rows)
        copies.append(
            remote(
                s.proj.at[rows], s.rows_in.at[place.tp],
                s.xa_send.at[k], s.xa_recv.at[k], {"tp": peers(k)},
            )
        )
    s.rows_in[place.tp] = s.proj[mine, :]
    for copy in copies:
        copy.wait_recv()
    per_device = s.proj.shape[1] // HD
    cos, sin = table[0], table[1]

    def head(h):
        column = (h % per_device) * HD
        return s.rows_in[h // per_device, :, column : column + HD]

    def turned(h):
        value = head(h).astype(F32)
        return (value * cos + pltpu.roll(value, HD // 2, 1) * sin).astype(BF16)

    for h in range(HEADS):
        s.queries[h * own_rows : (h + 1) * own_rows, :] = turned(h).astype(F32)
    for k in range(KV):
        s.keys[:, k * HD : (k + 1) * HD] = turned(HEADS + k)
        s.values[:, k * HD : (k + 1) * HD] = head(HEADS + KV + k)
    for r in range(own_rows):
        loads["row", r].wait()
    load("gate_up", 3, w_gate_up, gate_up)
    unroll = 4

    @pl.loop(0, own_rows // unroll)
    def _(i):
        for j in range(unroll):
            r = i * unroll + j
            strided = pl.ds(r, HEADS, stride=own_rows)
            s.attended[strided, :] = attend_row(
                region, r, s.queries[strided, :], s.keys[...], s.values[...],
                table[2, pl.ds(r, 1), :][:, :1], count, KV,
            )

    cols = lm_head.shape[1] // 2
    strip = pl.ds(pl.multiple_of(member * cols, cols), cols)
    piece = width // WORD_LOADS
    waiting.append(
        functools.partial(load, "down_0", 4, w_down.at[:, pl.ds(0, half)], region.at[pl.ds(width, ff)])
    )
    waiting.append(
        functools.partial(
            load, "down_1", 5, w_down.at[:, pl.ds(half, half)], region.at[pl.ds(width + ff, ff)]
        )
    )
    for i in range(WORD_LOADS):
        rows = pl.ds(i * piece, piece)
        waiting.append(
            functools.partial(
                load, ("words", i), 6 + own_rows + i, lm_head.at[rows, strip], region.at[rows]
            )
        )
    own_heads = w_out.shape[0] // HD
    for d in range(tp_count):
        for i in range(own_heads):
            h = d * own_heads + i
            s.heads_out[d, :, i * HD : (i + 1) * HD] = s.attended[
                h * own_rows : (h + 1) * own_rows, :
            ].astype(BF16)
    for copy in copies:
        copy.wait_send()
    copies = []
    for k in range(1, tp_count):
        copies.append(
            remote(
                s.heads_out.at[peers(k)], s.heads_in.at[mine],
                s.xb_send.at[k], s.xb_recv.at[k], {"tp": peers(k)},
            )
        )
    s.heads_in[mine, :] = s.heads_out[place.tp]
    loads["out"].wait()
    for copy in copies:
        copy.wait_recv()
    part, total = s.part, s.total
    sums = [s.got_dx, s.got_dy, s.put_x, s.put_y, s.got_x, s.got_y, s.put_z, s.got_z]

    def project_out(start, size):
        span = pl.ds(start, size)
        part[:, span] = jnp.dot(
            s.heads_in[...], s.w_out[:, span], preferred_element_type=F32
        ).astype(BF16)

    Reduce(place, part, total, own_rows, spans, (s.ra_send, s.ra_recv), sums).run(project_out, feed)
    while waiting:
        feed()
    for copy in copies:
        copy.wait_send()
    middle = s.middle
    middle[...] = (s.stream[...].astype(F32) + total[...]).astype(BF16)
    block[mine, :] = norm_rows(middle[...].astype(F32), gains[...][1:2]).astype(BF16)
    members, batch = 2, s.final.shape[1]
    acts, hidden = s.acts, s.hidden
    waited_up = []

    def gate_and_up(start, size):
        if not waited_up:
            loads["gate_up"].wait()
            acts[...] = jnp.zeros_like(acts)
            waited_up.append(True)
        wide = 256

        @pl.loop(0, size // wide)
        def _(i):
            span = pl.ds(pl.multiple_of(start + i * wide, wide), wide)
            values = block[:, span].astype(F32)
            for j in range(2):
                scaled = jnp.concatenate(
                    [
                        values[m * batch : (m + 1) * batch] * fast_in[m, :, span][j : j + 1]
                        for m in range(members)
                    ],
                    axis=0,
                ).astype(BF16)
                acts[j] += jnp.dot(scaled, gate_up[j, span, :], preferred_element_type=F32)

    Gather(place, block, own_rows, parts, side, (s.gb_send, s.gb_recv)).run(gate_and_up)
    for m in range(members):
        rows = slice(m * batch, (m + 1) * batch)
        gate = acts[0, rows, :] * fast_hidden[m][0:1]
        hidden[rows, :] = (
            gate / (1.0 + jnp.exp(-gate))
            * (acts[1, rows, :] * fast_hidden[m][1:2])
            * fast_hidden[m][2:3]
        ).astype(BF16)
    loads["down_0"].wait()
    loads["down_1"].wait()

    def project_down(start, size):
        side = start // half
        rows = pl.ds(width + side * ff, ff)
        part[:, pl.ds(start, size)] = jnp.dot(
            hidden[...], region[rows, pl.ds(start - side * half, size)],
            preferred_element_type=F32,
        ).astype(BF16)

    Reduce(place, part, total, own_rows, spans, (s.rb_send, s.rb_recv), sums).run(project_down)
    own_member = place.tp * own_rows // batch
    scale = jnp.where(own_member == 0, fast_out[...][0:1], fast_out[...][1:2])
    layer_out = (middle[...].astype(F32) + total[...] * scale).astype(BF16)
    s.own[...] = norm_rows(layer_out.astype(F32), gains[...][2:3]).astype(BF16)
    first = member == 0
    low, high = s.own[:, :half].astype(F32), s.own[:, half:].astype(F32)
    half_own, pair = s.half_own, s.pair
    half_own[...] = jnp.where(first, low, high)
    s.away[...] = jnp.where(first, high, low).astype(BF16)
    core = remote(s.away, s.from_core, s.side_send.at[0], s.side_recv.at[0], other)
    core.wait_recv()
    half_own[...] = half_own[...] + s.from_core[...].astype(F32)
    pair[...] = half_own[...].astype(BF16)
    twin = remote(
        pair, s.from_pair, s.side_send.at[1], s.side_recv.at[1], place.to_line(lines // 2)
    )
    twin.wait_recv()
    turn = 1 - 2 * lax.rem(place.line, 2)

    class Pairwise:
        lines = 2
        quad, quad_x, quad_y = place.quad, place.quad_x, place.quad_y
        to_x, to_y = place.to_x, place.to_y

        @staticmethod
        def line_at(step):
            return lax.rem(place.line + abs(step), 2)

        @staticmethod
        def to_line(step):
            return {"tp": (place.line + turn) * QUAD + place.quad}

    final = s.final
    at = lax.rem(place.line, 2) * QUAD + place.quad
    final[member, pl.ds(pl.multiple_of(at * own_rows, own_rows), own_rows), :] = (
        (half_own[...] + s.from_pair[...].astype(F32)) * 0.25
    ).astype(BF16)
    words = region.at[pl.ds(0, width)]
    shares = []

    def share(start, size):
        view = final.at[member, :, pl.ds(start, size)]
        shares.append(
            remote(
                view, view, s.share_send.at[len(shares)], s.share_recv.at[len(shares)], other
            )
        )

    last = half // 2
    PairGather(
        Pairwise, final.at[member], own_rows, [(0, last), (last, last)], (s.gc_send, s.gc_recv)
    ).run(share)
    for i in range(WORD_LOADS):
        loads["words", i].wait()
    for copy in shares:
        copy.wait_recv()
    tile_count = s.tile_send.shape[0]
    tile_width = cols // tile_count
    column = lax.broadcasted_iota(jnp.int32, (batch, batch), 1)
    corner = lax.broadcasted_iota(jnp.int32, (batch, batch), 0) == column
    wanted = jnp.sum(
        jnp.where(corner, targets[...].astype(F32), 0.0), axis=-1, keepdims=True
    ).astype(jnp.int32)
    peak = jnp.full((batch, 1), -jnp.inf, F32)
    amount = jnp.zeros((batch, 1), F32)
    found = jnp.zeros((batch, 1), F32)
    tiles = []
    for i in range(tile_count):
        span = pl.ds(i * tile_width, tile_width)
        tile = jnp.dot(final[0], words[:half, span], preferred_element_type=F32) + jnp.dot(
            final[1], words[half:, span], preferred_element_type=F32
        )
        into = out.at[:, pl.ds(pl.multiple_of(member * cols + i * tile_width, tile_width), tile_width)]
        into[...] = tile.astype(BF16)
        tiles.append(remote(into, into, s.tile_send.at[i], s.tile_recv.at[i], other))
        new = jnp.maximum(peak, jnp.max(tile, axis=-1, keepdims=True))
        amount = amount * jnp.exp(peak - new) + jnp.sum(
            jnp.exp(tile - new), axis=-1, keepdims=True
        )
        peak = new
        column = (
            (place.tp * 2 + member) * cols
            + i * tile_width
            + lax.broadcasted_iota(jnp.int32, tile.shape, 1)
        )
        found = found + jnp.sum(jnp.where(column == wanted, tile, 0.0), axis=-1, keepdims=True)
    lane = lax.broadcasted_iota(jnp.int32, (batch, 128), 1)
    facts = jnp.where(lane == 0, peak, jnp.where(lane == 1, amount, found))
    stats, board = s.stats, s.board
    stats[...] = jnp.transpose(facts)[:8, :]
    copies = []
    for slot, device in enumerate(others):
        copies.append(
            remote(
                stats, board.at[slot + 1], s.stat_send.at[slot], s.stat_recv.at[slot], device
            )
        )
    board[0] = stats[...]
    for copy in copies:
        copy.wait_recv()
    top = jnp.max(board[:, 0, :], axis=0, keepdims=True)
    amount = jnp.sum(board[:, 1, :] * jnp.exp(board[:, 0, :] - top), axis=0, keepdims=True)
    found = jnp.sum(board[:, 2, :], axis=0, keepdims=True)
    logprob[...] = found - (top + jnp.log(amount))
    for copy in tiles:
        copy.wait_recv()
    for copy in [core, twin] + shares + tiles + copies:
        copy.wait_send()


VMEM = pl.BlockSpec(memory_space=pltpu.VMEM)
ANY = pl.BlockSpec(memory_space=pl.ANY)


def fused_body(
    stream_in,
    kv_cache,
    lengths,
    targets,
    norm_gains,
    w_qkv,
    w_out,
    w_gate_up,
    w_down,
    lm_head,
    fast_in,
    fast_hidden,
    fast_out,
):
    tp_count = lax.axis_size("tp")
    tp_rank = lax.axis_index("tp")
    lines = tp_count // QUAD
    batch = lengths.shape[0]
    own_rows, width = stream_in.shape
    all_rows = own_rows * tp_count
    half = width // 2
    devices = 2 * tp_count
    vocab_cols = lm_head.shape[1]
    ff = w_down.shape[0]
    positions = lax.dynamic_slice_in_dim(
        lengths, (tp_rank * own_rows) % batch, own_rows, 0
    ).astype(F32)
    frequency = ROPE_BASE ** (-jnp.arange(HD // 2, dtype=F32) * 2.0 / HD)
    angles = positions[:, None] * frequency[None, :]
    cos, sin = jnp.cos(angles), jnp.sin(angles)
    table = jnp.stack(
        [
            jnp.concatenate([cos, cos], axis=1),
            jnp.concatenate([-sin, sin], axis=1),
            jnp.broadcast_to(positions[:, None], (own_rows, HD)),
        ]
    )
    tiles = 4
    small = pltpu.VMEM((lines, own_rows, half), BF16)
    large = pltpu.VMEM((lines, own_rows, width), BF16)
    own = pltpu.VMEM((own_rows, width), BF16)
    gather_out = DMA((7, lines, CHUNKS + 1))
    gather_in = DMA((5, lines, CHUNKS + 1))
    reduce = DMA((7, lines, CHUNKS))
    scratch = dict(
        region=pltpu.VMEM((own_rows * kv_cache.shape[1], kv_cache.shape[2]), BF16),
        gate_up=pltpu.VMEM(w_gate_up.shape, BF16),
        w_out=pltpu.VMEM(w_out.shape, BF16),
        block=pltpu.VMEM((all_rows, width), BF16),
        part=pltpu.VMEM((all_rows, width), BF16),
        stream=own,
        own=own,
        middle=own,
        total=pltpu.VMEM((own_rows, width), F32),
        proj=pltpu.VMEM((all_rows, w_qkv.shape[1]), BF16),
        rows_in=pltpu.VMEM((tp_count, own_rows, w_qkv.shape[1]), BF16),
        queries=pltpu.VMEM(((HEADS + 1) * own_rows, HD), F32),
        keys=pltpu.VMEM((own_rows, KV * HD), BF16),
        values=pltpu.VMEM((own_rows, KV * HD), BF16),
        attended=pltpu.VMEM(((HEADS + 1) * own_rows, HD), F32),
        heads_out=pltpu.VMEM((tp_count, own_rows, w_out.shape[0]), BF16),
        heads_in=pltpu.VMEM((all_rows, w_out.shape[0]), BF16),
        acts=pltpu.VMEM((2, all_rows, ff), F32),
        hidden=pltpu.VMEM((all_rows, ff), BF16),
        half_own=pltpu.VMEM((own_rows, half), F32),
        away=pltpu.VMEM((own_rows, half), BF16),
        from_core=pltpu.VMEM((own_rows, half), BF16),
        pair=pltpu.VMEM((own_rows, half), BF16),
        from_pair=pltpu.VMEM((own_rows, half), BF16),
        final=pltpu.VMEM((2, batch, half), BF16),
        stats=pltpu.VMEM((8, batch), F32),
        board=pltpu.VMEM((devices, 8, batch), F32),
        got_dx=small, got_dy=small, put_x=small, put_y=small,
        got_x=large, got_y=large, put_z=large, got_z=large,
        loads=DMA((6 + own_rows + WORD_LOADS,)),
        ga_send=gather_out, ga_recv=gather_in, gb_send=gather_out, gb_recv=gather_in,
        ra_send=reduce, ra_recv=reduce, rb_send=reduce, rb_recv=reduce,
        gc_send=DMA((5, 2, 2)), gc_recv=DMA((5, 2, 2)),
        xa_send=DMA((tp_count,)), xa_recv=DMA((tp_count,)),
        xb_send=DMA((tp_count,)), xb_recv=DMA((tp_count,)),
        side_send=DMA((2,)), side_recv=DMA((2,)),
        share_send=DMA((2,)), share_recv=DMA((2,)),
        tile_send=DMA((tiles,)), tile_recv=DMA((tiles,)),
        stat_send=DMA((devices,)), stat_recv=DMA((devices,)),
    )
    mean_logits, logprob = pl.pallas_call(
        functools.partial(layer_kernel, lines, tuple(scratch)),
        out_shape=[
            jax.ShapeDtypeStruct((batch, vocab_cols), BF16),
            jax.ShapeDtypeStruct((1, batch), F32),
        ],
        in_specs=[ANY] * 7 + [VMEM] * 6,
        out_specs=[VMEM, VMEM],
        scratch_shapes=list(scratch.values()),
        compiler_params=pltpu.CompilerParams(
            collective_id=1, has_side_effects=True, vmem_limit_bytes=VMEM_BYTES
        ),
    )(
        stream_in, kv_cache, w_qkv, w_out, w_gate_up, w_down, lm_head,
        table, norm_gains, fast_in, fast_hidden, fast_out, targets[None, :],
    )
    return (mean_logits, logprob[0])


VMEM_BYTES = 67043328


def body(*args):
    stream_in, kv_cache, lengths = args[0], args[1], args[2]
    w_qkv, w_out, w_down, lm_head, fast_in = args[5], args[6], args[8], args[9], args[10]
    own_rows, width = stream_in.shape
    batch, ff = lengths.shape[0], w_down.shape[0]
    tp_count = lax.axis_size("tp")
    fits = (
        tp_count == 4 * QUAD
        and own_rows == 16
        and batch == 128
        and lax.axis_size("member") == 2
        and fast_in.shape[0] == 2
        and own_rows * tp_count == 2 * batch
        and w_qkv.shape[1] % HD == 0
        and w_out.shape[0] % HD == 0
        and w_qkv.shape[1] <= ff
        and width % 4096 == 0
        and kv_cache.shape[2] * 2 == width
        and lm_head.shape[1] == width
        and own_rows * kv_cache.shape[1] >= width + 2 * ff
    )
    if fits:
        return fused_body(*args)
    return plain_body(*args)


def solution(mesh):
    in_specs = (
        P(("member", "tp"), None),
        P(("member", "tp"), None, None),
        P(),
        P(),
        P(),
        P(None, "tp"),
        P("tp", None),
        P(None, None, "tp"),
        P("tp", None),
        P(None, "tp"),
        P("member", None, None),
        P("member", None, "tp"),
        P("member", None),
    )
    out_specs = (P(None, "tp"), P())
    return jax.shard_map(body, mesh=mesh, in_specs=in_specs, out_specs=out_specs, check_vma=False)
```

```python
import functools
from types import SimpleNamespace

import jax
import jax.numpy as jnp
from jax import lax
from jax.experimental import pallas as pl
from jax.experimental.pallas import tpu as pltpu
from jax.sharding import PartitionSpec as P

HEADS = 32
KV = 8
HD = 128
CACHE = 512


ROPE_BASE = 500000.0


def rms_norm(values_in, gain):
    return (
        values_in
        * lax.rsqrt(jnp.mean(values_in * values_in, axis=-1, keepdims=True) + 1e-05)
        * gain
    )


def rotate(values_in, positions):
    half_dim = values_in.shape[-1] // 2
    frequency = ROPE_BASE ** (-jnp.arange(half_dim, dtype=jnp.float32) * 2.0 / values_in.shape[-1])
    angles = positions.astype(jnp.float32)[:, None, None] * frequency[None, None, :]
    lower_half = values_in[..., :half_dim]
    upper_half = values_in[..., half_dim:]
    return jnp.concatenate(
        [
            lower_half * jnp.cos(angles) - upper_half * jnp.sin(angles),
            upper_half * jnp.cos(angles) + lower_half * jnp.sin(angles),
        ],
        axis=-1,
    )


def attend(projected, cache_rows, positions):
    row_count = projected.shape[0]
    head_cols = HEADS * HD
    kv_cols = KV * HD
    queries = rotate(
        projected[:, :head_cols].astype(jnp.float32).reshape(row_count, HEADS, HD), positions
    ).astype(jnp.bfloat16)
    new_key = rotate(
        projected[:, head_cols : head_cols + kv_cols]
        .astype(jnp.float32)
        .reshape(row_count, KV, HD),
        positions,
    ).astype(jnp.bfloat16)
    new_value = projected[:, head_cols + kv_cols :].reshape(row_count, KV, HD)
    cache_keys = cache_rows[:, :, :kv_cols].reshape(row_count, CACHE, KV, HD)
    cache_values = cache_rows[:, :, kv_cols:].reshape(row_count, CACHE, KV, HD)
    grouped = queries.reshape(row_count, KV, HEADS // KV, HD)
    inv_root = HD ** (-0.5)
    cached = (
        jnp.einsum("rkgd,rckd->rkgc", grouped, cache_keys, preferred_element_type=jnp.float32)
        * inv_root
    )
    fresh = (
        jnp.einsum("rkgd,rkd->rkg", grouped, new_key, preferred_element_type=jnp.float32) * inv_root
    )
    in_cache = jnp.arange(CACHE)[None, :] < positions[:, None]
    cached = jnp.where(in_cache[:, None, None, :], cached, -1e30)
    peak = jnp.maximum(jnp.max(cached, axis=-1), fresh)
    weights = jnp.exp(cached - peak[..., None])
    fresh_w = jnp.exp(fresh - peak)
    total_sum = jnp.sum(weights, axis=-1) + fresh_w
    probs = (weights / total_sum[..., None]).astype(jnp.bfloat16)
    fresh_p = (fresh_w / total_sum).astype(jnp.bfloat16)
    result = jnp.einsum("rkgc,rckd->rkgd", probs, cache_values, preferred_element_type=jnp.float32)
    result = (
        result
        + fresh_p.astype(jnp.float32)[..., None] * new_value.astype(jnp.float32)[:, :, None, :]
    )
    return result.reshape(row_count, HEADS * HD).astype(jnp.bfloat16)


def plain_body(
    stream_in,
    kv_cache,
    lengths,
    targets,
    norm_gains,
    w_qkv,
    w_out,
    w_gate_up,
    w_down,
    lm_head,
    fast_in,
    fast_hidden,
    fast_out,
):
    tp_count = lax.axis_size("tp")
    tp_rank = lax.axis_index("tp")
    mem_dev = fast_in.shape[0]
    batch_rows = lengths.shape[0]
    own_rows = stream_in.shape[0]
    all_rows = own_rows * tp_count
    width = stream_in.shape[1]
    first_row = tp_rank * own_rows
    positions = lax.dynamic_slice_in_dim(lengths, first_row % batch_rows, own_rows, 0)
    own_member = first_row // batch_rows
    own_scale = lax.dynamic_index_in_dim(fast_out, own_member, 0, keepdims=True)
    own_normed = rms_norm(stream_in.astype(jnp.float32), norm_gains[0]).astype(jnp.bfloat16)
    attn_in = lax.all_gather(own_normed, "tp", axis=0, tiled=True)
    projected = jnp.dot(attn_in, w_qkv, preferred_element_type=jnp.float32).astype(jnp.bfloat16)
    row_major = lax.all_to_all(projected, "tp", split_axis=0, concat_axis=1, tiled=True)
    attended = attend(row_major, kv_cache, positions)
    head_major = lax.all_to_all(attended, "tp", split_axis=1, concat_axis=0, tiled=True)
    picked = head_major
    attn_sum = lax.psum_scatter(
        jnp.dot(picked, w_out, preferred_element_type=jnp.float32),
        "tp",
        scatter_dimension=0,
        tiled=True,
    )
    middle = (stream_in.astype(jnp.float32) + attn_sum).astype(jnp.bfloat16)
    own_ffn = rms_norm(middle.astype(jnp.float32), norm_gains[1]).astype(jnp.bfloat16)
    ffn_in = lax.all_gather(own_ffn, "tp", axis=0, tiled=True)
    grouped = ffn_in.astype(jnp.float32).reshape(mem_dev, batch_rows, width)
    gate_in = (grouped * fast_in[:, 0][:, None, :]).astype(jnp.bfloat16).reshape(all_rows, width)
    up_in = (grouped * fast_in[:, 1][:, None, :]).astype(jnp.bfloat16).reshape(all_rows, width)
    hidden_cols = w_gate_up.shape[2]
    gate_act = (
        jnp.dot(gate_in, w_gate_up[0], preferred_element_type=jnp.float32).reshape(
            mem_dev, batch_rows, hidden_cols
        )
        * fast_hidden[:, 0][:, None, :]
    )
    up_act = (
        jnp.dot(up_in, w_gate_up[1], preferred_element_type=jnp.float32).reshape(
            mem_dev, batch_rows, hidden_cols
        )
        * fast_hidden[:, 1][:, None, :]
    )
    hidden = (
        (jax.nn.silu(gate_act) * up_act * fast_hidden[:, 2][:, None, :])
        .astype(jnp.bfloat16)
        .reshape(all_rows, hidden_cols)
    )
    picked = hidden
    down_sum = lax.psum_scatter(
        jnp.dot(picked, w_down, preferred_element_type=jnp.float32),
        "tp",
        scatter_dimension=0,
        tiled=True,
    )
    layer_out = (middle.astype(jnp.float32) + down_sum * own_scale).astype(jnp.bfloat16)
    own_final = rms_norm(layer_out.astype(jnp.float32), norm_gains[2]).astype(jnp.bfloat16)
    final_in = lax.all_gather(own_final, "tp", axis=0, tiled=True)
    logits = jnp.dot(final_in, lm_head, preferred_element_type=jnp.float32)
    vocab_cols = lm_head.shape[1]
    member_total = jnp.sum(logits.reshape(mem_dev, batch_rows, vocab_cols), axis=0)
    member_count = mem_dev * lax.axis_size("member")
    mean_logit = (
        lax.psum(member_total.astype(jnp.bfloat16), "member").astype(jnp.float32) / member_count
    )
    column_ids = tp_rank * vocab_cols + jnp.arange(vocab_cols)
    target_part = jnp.sum(
        jnp.where(column_ids[None, :] == targets[:, None], mean_logit, 0.0), axis=-1
    )
    local_peak = jnp.max(mean_logit, axis=-1)
    peak = lax.pmax(local_peak, "tp")
    exp_total, target_logit = lax.psum(
        (jnp.sum(jnp.exp(mean_logit - peak[:, None]), axis=-1), target_part), "tp"
    )
    token_logprob = target_logit - (peak + jnp.log(exp_total))
    return (mean_logit.astype(jnp.bfloat16), token_logprob)


BF16 = jnp.bfloat16
F32 = jnp.float32
DMA = pltpu.SemaphoreType.DMA
QUAD = 4


def norm_rows(values_in, gain):
    return (
        values_in
        * lax.rsqrt(jnp.mean(values_in * values_in, axis=-1, keepdims=True) + 1e-05)
        * gain
    )


class Place:
    def __init__(self, lines):
        self.tp = lax.axis_index("tp")
        self.member = lax.axis_index("member")
        self.lines = lines
        self.quad = lax.rem(self.tp, QUAD)
        self.line = self.tp // QUAD
        self.quad_x = self.quad + 1 - 2 * lax.rem(self.quad, 2)
        self.quad_y = lax.rem(self.quad + 2, QUAD)
        self.quad_d = self.quad_x + self.quad_y - self.quad
        self.to_x = {"tp": self.line * QUAD + self.quad_x}
        self.to_y = {"tp": self.line * QUAD + self.quad_y}
        self.inner = jnp.logical_or(self.line == 1, self.line == 2)
        beside, across, over = (
            self.line + 1 - 2 * lax.rem(self.line, 2),
            lines - 1 - self.line,
            lax.rem(self.line + 2, lines),
        )
        self.near = [
            self.line,
            beside,
            jnp.where(self.inner, across, over),
            jnp.where(self.inner, over, across),
        ]
        self.pair = {"tp": beside * QUAD + self.quad}
        self.middle = {"tp": across * QUAD + self.quad}

    def line_at(self, step):
        return lax.rem(self.line + step + self.lines, self.lines)

    def to_line(self, step):
        return {"tp": self.line_at(step) * QUAD + self.quad}


def remote(src, dst, send_sem, recv_sem, device):
    copy = pltpu.make_async_remote_copy(
        src_ref=src,
        dst_ref=dst,
        send_sem=send_sem,
        recv_sem=recv_sem,
        device_id=device,
        device_id_type=pl.DeviceIdType.MESH,
    )
    copy.start()
    return copy


NT = (((1,), (1,)), ((), ()))
CHUNKS = 2
WORD_LOADS = 8


class PairGather:
    def __init__(self, place, buf, rows, spans, sems):
        self.place, self.buf, self.rows, self.spans = place, buf, rows, spans
        self.sends, self.recvs = sems
        self.copies = {}

    def at(self, step, quad, start, width):
        index = self.place.line_at(step) * QUAD + quad
        rows = pl.ds(pl.multiple_of(index * self.rows, self.rows), self.rows)
        return self.buf.at[rows, pl.ds(start, width)]

    def send(self, kind, k, c, block, device):
        self.copies[kind, k, c] = remote(
            block, block, self.sends.at[kind, k, c], self.recvs.at[kind, k, c], device
        )

    def start(self):
        place = self.place
        for c, (start, width) in enumerate(self.spans):
            mine = self.at(0, place.quad, start, width)
            for k in range(1, place.lines):
                self.send(0, k, c, mine, place.to_line(k))
            self.send(1, 0, c, mine, place.to_x)
            self.send(2, 0, c, mine, place.to_y)

    def spread(self, c):
        place = self.place
        for k in range(1, place.lines):
            self.copies[0, k, c].wait_recv()
            block = self.at(-k, place.quad, *self.spans[c])
            self.send(1, k, c, block, place.to_x)
            self.send(2, k, c, block, place.to_y)
            self.feed()

    def relay(self, c):
        place = self.place
        start, width = self.spans[c]
        half = width // 2
        for k in range(place.lines):
            self.copies[1, k, c].wait_recv()
            self.send(3, k, c, self.at(-k, place.quad_x, start, half), place.to_y)
            self.copies[2, k, c].wait_recv()
            self.send(4, k, c, self.at(-k, place.quad_y, start + half, half), place.to_x)
            self.feed()

    def arrive(self, c):
        for k in range(self.place.lines):
            self.copies[3, k, c].wait_recv()
            self.copies[4, k, c].wait_recv()

    def run(self, compute, feed=lambda: None):
        count = len(self.spans)
        self.feed = feed
        self.start()
        self.spread(0)
        for c in range(count):
            if c + 1 < count:
                self.spread(c + 1)
            self.relay(c)
            if c:
                self.arrive(c - 1)
                compute(*self.spans[c - 1])
        self.arrive(count - 1)
        compute(*self.spans[count - 1])
        for copy in self.copies.values():
            copy.wait_send()


class Gather:
    def __init__(self, place, buf, rows, spans, side, sems):
        self.place, self.buf, self.rows = place, buf, rows
        self.spans, self.side = spans, side
        self.sends, self.recvs = sems
        self.copies, self.guarded = {}, []

    def at(self, line, quad, start, width):
        index = line * QUAD + quad
        rows = pl.ds(pl.multiple_of(index * self.rows, self.rows), self.rows)
        return self.buf.at[rows, pl.ds(start, width)]

    def plane(self, line, start, width):
        rows = QUAD * self.rows
        return self.buf.at[pl.ds(pl.multiple_of(line * rows, rows), rows), pl.ds(start, width)]

    def send(self, kind, k, c, block, device):
        self.copies[kind, k, c] = remote(
            block, block, self.sends.at[kind, k, c], self.recvs.at[kind, k, c], device
        )

    def cross(self, slot, k, c, block, device, inner):
        copy = pltpu.make_async_remote_copy(
            src_ref=block, dst_ref=block,
            send_sem=self.sends.at[slot, k, c], recv_sem=self.recvs.at[0, slot_of(slot, k), c],
            device_id=device, device_id_type=pl.DeviceIdType.MESH,
        )
        if inner:
            self.guarded.append(copy)

            @pl.when(self.place.inner)
            def _():
                copy.start()
        else:
            copy.start()
            self.copies[slot, k, c] = copy

    def await_line(self, k, c, block):
        pltpu.make_async_remote_copy(
            src_ref=block, dst_ref=block,
            send_sem=self.sends.at[0, k, c], recv_sem=self.recvs.at[0, k, c],
            device_id=self.place.pair, device_id_type=pl.DeviceIdType.MESH,
        ).wait_recv()

    def own_line(self, c, block):
        self.cross(5, 0, c, block, self.place.pair, False)
        self.cross(6, 0, c, block, self.place.middle, True)

    def pass_line(self, k, c, block):
        if k == 1:
            self.cross(6, 1, c, block, self.place.middle, True)
        else:
            self.cross(5, k - 1, c, block, self.place.pair, True)

    def start(self):
        place = self.place
        count = len(self.spans)
        for c, span in enumerate(self.spans):
            self.own_line(c, self.at(place.line, place.quad, *span))
        for c, span in [(count, self.side)] + list(enumerate(self.spans)):
            mine = self.at(place.line, place.quad, *span)
            self.send(1, 0, c, mine, place.to_x)
            self.send(2, 0, c, mine, place.to_y)

    def spread(self, c):
        place = self.place
        for k in range(1, place.lines):
            block = self.at(place.near[k], place.quad, *self.spans[c])
            self.await_line(k, c, block)
            self.pass_line(k, c, block)
            self.send(1, k, c, block, place.to_x)
            self.send(2, k, c, block, place.to_y)
            self.feed()

    def relay(self, c, k):
        place = self.place
        start, width = (self.spans + [self.side])[c]
        half = width // 256 * 128
        self.copies[1, k, c].wait_recv()
        self.send(3, k, c, self.at(place.near[k], place.quad_x, start, half), place.to_y)
        self.copies[2, k, c].wait_recv()
        self.send(
            4, k, c, self.at(place.near[k], place.quad_y, start + half, width - half), place.to_x
        )

    def arrive(self, c):
        for k in range(self.place.lines):
            self.copies[3, k, c].wait_recv()
            self.copies[4, k, c].wait_recv()

    def side_step(self, k):
        c = len(self.spans)
        if k == 0:
            self.copies[3, 0, c].wait_recv()
            self.copies[4, 0, c].wait_recv()
            self.own_line(c, self.plane(self.place.line, *self.side))
        else:
            block = self.plane(self.place.near[k], *self.side)
            self.await_line(k, c, block)
            self.pass_line(k, c, block)

    def run(self, compute, feed=lambda: None):
        place = self.place
        count = len(self.spans)
        self.feed = feed
        self.start()
        self.relay(count, 0)
        self.spread(0)
        self.side_step(0)
        for c in range(count):
            if c + 1 < count:
                self.spread(c + 1)
            if c:
                self.side_step(c)
            for k in range(place.lines):
                self.relay(c, k)
                self.feed()
            if c:
                self.arrive(c - 1)
                compute(*self.spans[c - 1])
        for k in range(count, place.lines):
            self.side_step(k)
        compute(*self.side)
        self.arrive(count - 1)
        compute(*self.spans[count - 1])
        for copy in self.copies.values():
            copy.wait_send()

        @pl.when(place.inner)
        def _():
            for copy in self.guarded:
                copy.wait_send()


def slot_of(slot, k):
    if slot == 5:
        return k + 1
    return k + 2


class Reduce:
    def __init__(self, place, part, total, rows, spans, sems, bufs):
        self.place, self.part, self.total = place, part, total
        self.rows, self.spans = rows, spans
        self.sends, self.recvs = sems
        self.got_dx, self.got_dy, self.put_x, self.put_y = bufs[:4]
        self.got_x, self.got_y, self.put_z, self.got_z = bufs[4:]
        self.steps = list(range(1, place.lines)) + [0]
        self.copies = {}

    def at(self, step, quad):
        index = self.place.line_at(step) * QUAD + quad
        return pl.ds(pl.multiple_of(index * self.rows, self.rows), self.rows)

    def send(self, kind, k, c, src, dst, device):
        self.copies[kind, k, c] = remote(
            src, dst, self.sends.at[kind, k, c], self.recvs.at[kind, k, c], device
        )

    def halves(self, c):
        start, width = self.spans[c]
        return pl.ds(start, width // 2), pl.ds(start + width // 2, width // 2)

    def packed(self, c):
        start, width = self.spans[c]
        return pl.ds(start // 2, width // 2)

    def direct(self, c):
        place, part = self.place, self.part
        low, high = self.halves(c)
        packed = self.packed(c)
        for k in self.steps:
            diag = self.at(k, place.quad_d)
            self.send(0, k, c, part.at[diag, high], self.got_dx.at[k, :, packed], place.to_x)
            self.send(1, k, c, part.at[diag, low], self.got_dy.at[k, :, packed], place.to_y)
        for k in self.steps:
            self.send(2, k, c, part.at[self.at(k, place.quad_x), high], self.got_x.at[k, :, high], place.to_x)
            self.send(3, k, c, part.at[self.at(k, place.quad_y), low], self.got_y.at[k, :, low], place.to_y)

    def follow(self, c):
        place, part = self.place, self.part
        low, high = self.halves(c)
        packed = self.packed(c)
        for k in self.steps:
            self.copies[1, k, c].wait_recv()
            self.put_x[k, :, packed] = (
                part[self.at(k, place.quad_x), low].astype(F32)
                + self.got_dy[k, :, packed].astype(F32)
            ).astype(BF16)
            self.send(4, k, c, self.put_x.at[k, :, packed], self.got_x.at[k, :, low], place.to_x)
            self.copies[0, k, c].wait_recv()
            self.put_y[k, :, packed] = (
                part[self.at(k, place.quad_y), high].astype(F32)
                + self.got_dx[k, :, packed].astype(F32)
            ).astype(BF16)
            self.send(5, k, c, self.put_y.at[k, :, packed], self.got_y.at[k, :, high], place.to_y)
            self.feed()

    def settle(self, c):
        place, part = self.place, self.part
        span = pl.ds(*self.spans[c])
        for k in self.steps:
            for kind in (2, 3, 4, 5):
                self.copies[kind, k, c].wait_recv()
            quad_sum = (
                part[self.at(k, place.quad), span].astype(F32)
                + self.got_x[k, :, span].astype(F32)
                + self.got_y[k, :, span].astype(F32)
            )
            if k:
                self.put_z[k, :, span] = quad_sum.astype(BF16)
                self.send(6, k, c, self.put_z.at[k, :, span], self.got_z.at[k, :, span], place.to_line(k))
            else:
                self.total[:, span] = quad_sum
            self.feed()

    def run(self, compute, feed=lambda: None):
        count = len(self.spans)
        self.feed = feed
        compute(*self.spans[0])
        self.direct(0)
        for c in range(count):
            if c + 1 < count:
                compute(*self.spans[c + 1])
            self.follow(c)
            if c + 1 < count:
                self.direct(c + 1)
            self.settle(c)
        for c in range(count):
            span = pl.ds(*self.spans[c])
            for k in self.steps[:-1]:
                self.copies[6, k, c].wait_recv()
                self.total[:, span] += self.got_z[k, :, span].astype(F32)
        for copy in self.copies.values():
            copy.wait_send()


def attend_row(region, row, query, fresh_keys, fresh_values, position, count, key_heads):
    head_size = query.shape[1]
    group = query.shape[0] // key_heads
    kv_cols = key_heads * head_size
    inv_root = head_size ** (-0.5)
    wide = jnp.concatenate([query] * key_heads, axis=1)
    owner = lax.broadcasted_iota(jnp.int32, wide.shape, 0) // group
    column = lax.broadcasted_iota(jnp.int32, wide.shape, 1) // head_size
    wide = jnp.where(owner == column, wide, 0.0).astype(BF16)
    span = pl.ds(pl.multiple_of(row * count, count), count)
    scores = lax.dot_general(wide, region[span, :kv_cols], NT, preferred_element_type=F32) * inv_root
    fresh = lax.dot_general(wide, fresh_keys, NT, preferred_element_type=F32) * inv_root
    spot = lax.broadcasted_iota(jnp.int32, scores.shape, 1).astype(F32)
    scores = jnp.where(spot < position, scores, -1e30)
    fresh = jnp.where(lax.broadcasted_iota(jnp.int32, fresh.shape, 1) == row, fresh, -1e30)
    peak = jnp.maximum(
        jnp.max(scores, axis=1, keepdims=True), jnp.max(fresh, axis=1, keepdims=True)
    )
    weights = jnp.exp(scores - peak)
    fresh_w = jnp.exp(fresh - peak)
    scale = 1.0 / (
        jnp.sum(weights, axis=1, keepdims=True) + jnp.sum(fresh_w, axis=1, keepdims=True)
    )
    full = jnp.dot(
        (weights * scale).astype(BF16), region[span, kv_cols:], preferred_element_type=F32
    ) + jnp.dot((fresh_w * scale).astype(BF16), fresh_values, preferred_element_type=F32)
    full = jnp.where(owner == column, full, 0.0)
    result = full[:, :head_size]
    for k in range(1, key_heads):
        result = result + full[:, k * head_size : (k + 1) * head_size]
    return result


def layer_kernel(
    lines, names, stream, cache, w_qkv, w_out, w_gate_up, w_down, lm_head,
    table, gains, fast_in, fast_hidden, fast_out, targets, out, logprob, *refs
):
    s = SimpleNamespace(**dict(zip(names, refs)))
    place = Place(lines)
    tp_count = lines * QUAD
    member = place.member
    other = {"member": 1 - member}
    own_rows, width = s.own.shape
    region, gate_up, block = s.region, s.gate_up, s.block
    count = cache.shape[1]
    ff = w_down.shape[0]
    half = width // 2

    loads = {}

    def load(name, i, src, dst):
        loads[name] = pltpu.make_async_copy(src, dst, s.loads.at[i])
        loads[name].start()

    barrier = pltpu.get_barrier_semaphore()
    others = []
    for core in (member, 1 - member):
        for step in range(tp_count):
            if others or step:
                others.append({"member": core, "tp": lax.rem(place.tp + step, tp_count)})
    for device in others:
        pl.semaphore_signal(barrier, inc=1, device_id=device, device_id_type=pl.DeviceIdType.MESH)
    load("stream", 0, stream, s.stream)
    qkv = gate_up.at[0, :, pl.ds(0, w_qkv.shape[1])]
    load("qkv", 1, w_qkv, qkv)
    waiting = [
        functools.partial(load, ("row", r), 6 + r, cache.at[r], region.at[pl.ds(r * count, count)])
        for r in range(own_rows)
    ]
    waiting.append(functools.partial(load, "out", 2, w_out, s.w_out))

    def feed():
        if waiting:
            waiting.pop(0)()

    loads["stream"].wait()
    mine = pl.ds(pl.multiple_of(place.tp * own_rows, own_rows), own_rows)
    block[mine, :] = norm_rows(s.stream[...].astype(F32), gains[...][0:1]).astype(BF16)
    pl.semaphore_wait(barrier, len(others))

    early = width * 5 // 8
    spans = [(0, early), (early, width - early)]
    eighth, last = width // 8, width * 5 // 16
    parts = [(0, width - eighth - last), (width - eighth - last, last)]
    side = (width - eighth, eighth)
    first_sums = s.acts.at[0, :, pl.ds(0, w_qkv.shape[1])]
    waited = []

    def project(start, size):
        if not waited:
            loads["qkv"].wait()
            waited.append(True)
        span = pl.ds(start, size)
        step = jnp.dot(block[:, span], qkv[span, :], preferred_element_type=F32)
        if start:
            first_sums[...] += step
        else:
            first_sums[...] = step

    Gather(place, block, own_rows, parts, side, (s.ga_send, s.ga_recv)).run(project, feed)
    while waiting:
        feed()
    s.proj[...] = first_sums[...].astype(BF16)

    def peers(k):
        return lax.rem(place.tp + k, tp_count)

    copies = []
    for k in range(1, tp_count):
        rows = pl.ds(pl.multiple_of(peers(k) * own_rows, own_rows), own_rows)
        copies.append(
            remote(
                s.proj.at[rows], s.rows_in.at[place.tp],
                s.xa_send.at[k], s.xa_recv.at[k], {"tp": peers(k)},
            )
        )
    s.rows_in[place.tp] = s.proj[mine, :]
    for copy in copies:
        copy.wait_recv()
    per_device = s.proj.shape[1] // HD
    cos, sin = table[0], table[1]

    def head(h):
        column = (h % per_device) * HD
        return s.rows_in[h // per_device, :, column : column + HD]

    def turned(h):
        value = head(h).astype(F32)
        return (value * cos + pltpu.roll(value, HD // 2, 1) * sin).astype(BF16)

    for h in range(HEADS):
        s.queries[h * own_rows : (h + 1) * own_rows, :] = turned(h).astype(F32)
    for k in range(KV):
        s.keys[:, k * HD : (k + 1) * HD] = turned(HEADS + k)
        s.values[:, k * HD : (k + 1) * HD] = head(HEADS + KV + k)
    for r in range(own_rows):
        loads["row", r].wait()
    load("gate_up", 3, w_gate_up, gate_up)
    unroll = 4

    @pl.loop(0, own_rows // unroll)
    def _(i):
        for j in range(unroll):
            r = i * unroll + j
            strided = pl.ds(r, HEADS, stride=own_rows)
            s.attended[strided, :] = attend_row(
                region, r, s.queries[strided, :], s.keys[...], s.values[...],
                table[2, pl.ds(r, 1), :][:, :1], count, KV,
            )

    cols = lm_head.shape[1] // 2
    strip = pl.ds(pl.multiple_of(member * cols, cols), cols)
    piece = width // WORD_LOADS
    waiting.append(
        functools.partial(load, "down_0", 4, w_down.at[:, pl.ds(0, half)], region.at[pl.ds(width, ff)])
    )
    waiting.append(
        functools.partial(
            load, "down_1", 5, w_down.at[:, pl.ds(half, half)], region.at[pl.ds(width + ff, ff)]
        )
    )
    for i in range(WORD_LOADS):
        rows = pl.ds(i * piece, piece)
        waiting.append(
            functools.partial(
                load, ("words", i), 6 + own_rows + i, lm_head.at[rows, strip], region.at[rows]
            )
        )
    own_heads = w_out.shape[0] // HD
    for d in range(tp_count):
        for i in range(own_heads):
            h = d * own_heads + i
            s.heads_out[d, :, i * HD : (i + 1) * HD] = s.attended[
                h * own_rows : (h + 1) * own_rows, :
            ].astype(BF16)
    for copy in copies:
        copy.wait_send()
    copies = []
    for k in range(1, tp_count):
        copies.append(
            remote(
                s.heads_out.at[peers(k)], s.heads_in.at[mine],
                s.xb_send.at[k], s.xb_recv.at[k], {"tp": peers(k)},
            )
        )
    s.heads_in[mine, :] = s.heads_out[place.tp]
    loads["out"].wait()
    for copy in copies:
        copy.wait_recv()
    part, total = s.part, s.total
    sums = [s.got_dx, s.got_dy, s.put_x, s.put_y, s.got_x, s.got_y, s.put_z, s.got_z]

    def project_out(start, size):
        span = pl.ds(start, size)
        part[:, span] = jnp.dot(
            s.heads_in[...], s.w_out[:, span], preferred_element_type=F32
        ).astype(BF16)

    Reduce(place, part, total, own_rows, spans, (s.ra_send, s.ra_recv), sums).run(project_out, feed)
    while waiting:
        feed()
    for copy in copies:
        copy.wait_send()
    middle = s.middle
    middle[...] = (s.stream[...].astype(F32) + total[...]).astype(BF16)
    block[mine, :] = norm_rows(middle[...].astype(F32), gains[...][1:2]).astype(BF16)
    members, batch = 2, s.final.shape[1]
    acts, hidden = s.acts, s.hidden
    waited_up = []

    def gate_and_up(start, size):
        if not waited_up:
            loads["gate_up"].wait()
            acts[...] = jnp.zeros_like(acts)
            waited_up.append(True)
        wide = 256

        @pl.loop(0, size // wide)
        def _(i):
            span = pl.ds(pl.multiple_of(start + i * wide, wide), wide)
            values = block[:, span].astype(F32)
            for j in range(2):
                scaled = jnp.concatenate(
                    [
                        values[m * batch : (m + 1) * batch] * fast_in[m, :, span][j : j + 1]
                        for m in range(members)
                    ],
                    axis=0,
                ).astype(BF16)
                acts[j] += jnp.dot(scaled, gate_up[j, span, :], preferred_element_type=F32)

    Gather(place, block, own_rows, parts, side, (s.gb_send, s.gb_recv)).run(gate_and_up)
    for m in range(members):
        rows = slice(m * batch, (m + 1) * batch)
        gate = acts[0, rows, :] * fast_hidden[m][0:1]
        hidden[rows, :] = (
            gate / (1.0 + jnp.exp(-gate))
            * (acts[1, rows, :] * fast_hidden[m][1:2])
            * fast_hidden[m][2:3]
        ).astype(BF16)
    loads["down_0"].wait()
    loads["down_1"].wait()

    def project_down(start, size):
        wide = 512
        for first in range(start, start + size, wide):
            strip_side = first // half
            rows = pl.ds(width + strip_side * ff, ff)
            part[:, pl.ds(first, wide)] = jnp.dot(
                hidden[...], region[rows, pl.ds(first - strip_side * half, wide)],
                preferred_element_type=F32,
            ).astype(BF16)

    Reduce(place, part, total, own_rows, spans, (s.rb_send, s.rb_recv), sums).run(project_down)
    own_member = place.tp * own_rows // batch
    scale = jnp.where(own_member == 0, fast_out[...][0:1], fast_out[...][1:2])
    layer_out = (middle[...].astype(F32) + total[...] * scale).astype(BF16)
    s.own[...] = norm_rows(layer_out.astype(F32), gains[...][2:3]).astype(BF16)
    first = member == 0
    low, high = s.own[:, :half].astype(F32), s.own[:, half:].astype(F32)
    half_own, pair = s.half_own, s.pair
    half_own[...] = jnp.where(first, low, high)
    s.away[...] = jnp.where(first, high, low).astype(BF16)
    core = remote(s.away, s.from_core, s.side_send.at[0], s.side_recv.at[0], other)
    core.wait_recv()
    half_own[...] = half_own[...] + s.from_core[...].astype(F32)
    pair[...] = half_own[...].astype(BF16)
    twin = remote(
        pair, s.from_pair, s.side_send.at[1], s.side_recv.at[1], place.to_line(lines // 2)
    )
    twin.wait_recv()
    turn = 1 - 2 * lax.rem(place.line, 2)

    class Pairwise:
        lines = 2
        quad, quad_x, quad_y = place.quad, place.quad_x, place.quad_y
        to_x, to_y = place.to_x, place.to_y

        @staticmethod
        def line_at(step):
            return lax.rem(place.line + abs(step), 2)

        @staticmethod
        def to_line(step):
            return {"tp": (place.line + turn) * QUAD + place.quad}

    final = s.final
    at = lax.rem(place.line, 2) * QUAD + place.quad
    final[member, pl.ds(pl.multiple_of(at * own_rows, own_rows), own_rows), :] = (
        (half_own[...] + s.from_pair[...].astype(F32)) * 0.25
    ).astype(BF16)
    words = region.at[pl.ds(0, width)]
    shares = []

    def share(start, size):
        view = final.at[member, :, pl.ds(start, size)]
        shares.append(
            remote(
                view, view, s.share_send.at[len(shares)], s.share_recv.at[len(shares)], other
            )
        )

    last = half // 2
    PairGather(
        Pairwise, final.at[member], own_rows, [(0, last), (last, last)], (s.gc_send, s.gc_recv)
    ).run(share)
    for i in range(WORD_LOADS):
        loads["words", i].wait()
    for copy in shares:
        copy.wait_recv()
    tile_count = s.tile_send.shape[0]
    tile_width = cols // tile_count
    column = lax.broadcasted_iota(jnp.int32, (batch, batch), 1)
    corner = lax.broadcasted_iota(jnp.int32, (batch, batch), 0) == column
    wanted = jnp.sum(
        jnp.where(corner, targets[...].astype(F32), 0.0), axis=-1, keepdims=True
    ).astype(jnp.int32)
    peak = jnp.full((batch, 1), -jnp.inf, F32)
    amount = jnp.zeros((batch, 1), F32)
    found = jnp.zeros((batch, 1), F32)
    tiles = []
    for i in range(tile_count):
        span = pl.ds(i * tile_width, tile_width)
        tile = jnp.dot(final[0], words[:half, span], preferred_element_type=F32) + jnp.dot(
            final[1], words[half:, span], preferred_element_type=F32
        )
        into = out.at[:, pl.ds(pl.multiple_of(member * cols + i * tile_width, tile_width), tile_width)]
        into[...] = tile.astype(BF16)
        tiles.append(remote(into, into, s.tile_send.at[i], s.tile_recv.at[i], other))
        new = jnp.maximum(peak, jnp.max(tile, axis=-1, keepdims=True))
        amount = amount * jnp.exp(peak - new) + jnp.sum(
            jnp.exp(tile - new), axis=-1, keepdims=True
        )
        peak = new
        column = (
            (place.tp * 2 + member) * cols
            + i * tile_width
            + lax.broadcasted_iota(jnp.int32, tile.shape, 1)
        )
        found = found + jnp.sum(jnp.where(column == wanted, tile, 0.0), axis=-1, keepdims=True)
    lane = lax.broadcasted_iota(jnp.int32, (batch, 128), 1)
    facts = jnp.where(lane == 0, peak, jnp.where(lane == 1, amount, found))
    stats, board = s.stats, s.board
    stats[...] = jnp.transpose(facts)[:8, :]
    copies = []
    for slot, device in enumerate(others):
        copies.append(
            remote(
                stats, board.at[slot + 1], s.stat_send.at[slot], s.stat_recv.at[slot], device
            )
        )
    board[0] = stats[...]
    for copy in copies:
        copy.wait_recv()
    top = jnp.max(board[:, 0, :], axis=0, keepdims=True)
    amount = jnp.sum(board[:, 1, :] * jnp.exp(board[:, 0, :] - top), axis=0, keepdims=True)
    found = jnp.sum(board[:, 2, :], axis=0, keepdims=True)
    logprob[...] = found - (top + jnp.log(amount))
    for copy in tiles:
        copy.wait_recv()
    for copy in [core, twin] + shares + tiles + copies:
        copy.wait_send()


VMEM = pl.BlockSpec(memory_space=pltpu.VMEM)
ANY = pl.BlockSpec(memory_space=pl.ANY)


def fused_body(
    stream_in,
    kv_cache,
    lengths,
    targets,
    norm_gains,
    w_qkv,
    w_out,
    w_gate_up,
    w_down,
    lm_head,
    fast_in,
    fast_hidden,
    fast_out,
):
    tp_count = lax.axis_size("tp")
    tp_rank = lax.axis_index("tp")
    lines = tp_count // QUAD
    batch = lengths.shape[0]
    own_rows, width = stream_in.shape
    all_rows = own_rows * tp_count
    half = width // 2
    devices = 2 * tp_count
    vocab_cols = lm_head.shape[1]
    ff = w_down.shape[0]
    positions = lax.dynamic_slice_in_dim(
        lengths, (tp_rank * own_rows) % batch, own_rows, 0
    ).astype(F32)
    frequency = ROPE_BASE ** (-jnp.arange(HD // 2, dtype=F32) * 2.0 / HD)
    angles = positions[:, None] * frequency[None, :]
    cos, sin = jnp.cos(angles), jnp.sin(angles)
    table = jnp.stack(
        [
            jnp.concatenate([cos, cos], axis=1),
            jnp.concatenate([-sin, sin], axis=1),
            jnp.broadcast_to(positions[:, None], (own_rows, HD)),
        ]
    )
    tiles = 4
    small = pltpu.VMEM((lines, own_rows, half), BF16)
    large = pltpu.VMEM((lines, own_rows, width), BF16)
    own = pltpu.VMEM((own_rows, width), BF16)
    gather_out = DMA((7, lines, CHUNKS + 1))
    gather_in = DMA((5, lines, CHUNKS + 1))
    reduce = DMA((7, lines, CHUNKS))
    scratch = dict(
        region=pltpu.VMEM((own_rows * kv_cache.shape[1], kv_cache.shape[2]), BF16),
        gate_up=pltpu.VMEM(w_gate_up.shape, BF16),
        w_out=pltpu.VMEM(w_out.shape, BF16),
        block=pltpu.VMEM((all_rows, width), BF16),
        part=pltpu.VMEM((all_rows, width), BF16),
        stream=own,
        own=own,
        middle=own,
        total=pltpu.VMEM((own_rows, width), F32),
        proj=pltpu.VMEM((all_rows, w_qkv.shape[1]), BF16),
        rows_in=pltpu.VMEM((tp_count, own_rows, w_qkv.shape[1]), BF16),
        queries=pltpu.VMEM(((HEADS + 1) * own_rows, HD), F32),
        keys=pltpu.VMEM((own_rows, KV * HD), BF16),
        values=pltpu.VMEM((own_rows, KV * HD), BF16),
        attended=pltpu.VMEM(((HEADS + 1) * own_rows, HD), F32),
        heads_out=pltpu.VMEM((tp_count, own_rows, w_out.shape[0]), BF16),
        heads_in=pltpu.VMEM((all_rows, w_out.shape[0]), BF16),
        acts=pltpu.VMEM((2, all_rows, ff), F32),
        hidden=pltpu.VMEM((all_rows, ff), BF16),
        half_own=pltpu.VMEM((own_rows, half), F32),
        away=pltpu.VMEM((own_rows, half), BF16),
        from_core=pltpu.VMEM((own_rows, half), BF16),
        pair=pltpu.VMEM((own_rows, half), BF16),
        from_pair=pltpu.VMEM((own_rows, half), BF16),
        final=pltpu.VMEM((2, batch, half), BF16),
        stats=pltpu.VMEM((8, batch), F32),
        board=pltpu.VMEM((devices, 8, batch), F32),
        got_dx=small, got_dy=small, put_x=small, put_y=small,
        got_x=large, got_y=large, put_z=large, got_z=large,
        loads=DMA((6 + own_rows + WORD_LOADS,)),
        ga_send=gather_out, ga_recv=gather_in, gb_send=gather_out, gb_recv=gather_in,
        ra_send=reduce, ra_recv=reduce, rb_send=reduce, rb_recv=reduce,
        gc_send=DMA((5, 2, 2)), gc_recv=DMA((5, 2, 2)),
        xa_send=DMA((tp_count,)), xa_recv=DMA((tp_count,)),
        xb_send=DMA((tp_count,)), xb_recv=DMA((tp_count,)),
        side_send=DMA((2,)), side_recv=DMA((2,)),
        share_send=DMA((2,)), share_recv=DMA((2,)),
        tile_send=DMA((tiles,)), tile_recv=DMA((tiles,)),
        stat_send=DMA((devices,)), stat_recv=DMA((devices,)),
    )
    mean_logits, logprob = pl.pallas_call(
        functools.partial(layer_kernel, lines, tuple(scratch)),
        out_shape=[
            jax.ShapeDtypeStruct((batch, vocab_cols), BF16),
            jax.ShapeDtypeStruct((1, batch), F32),
        ],
        in_specs=[ANY] * 7 + [VMEM] * 6,
        out_specs=[VMEM, VMEM],
        scratch_shapes=list(scratch.values()),
        compiler_params=pltpu.CompilerParams(
            collective_id=1, has_side_effects=True, vmem_limit_bytes=VMEM_BYTES
        ),
    )(
        stream_in, kv_cache, w_qkv, w_out, w_gate_up, w_down, lm_head,
        table, norm_gains, fast_in, fast_hidden, fast_out, targets[None, :],
    )
    return (mean_logits, logprob[0])


VMEM_BYTES = 67043328


def body(*args):
    stream_in, kv_cache, lengths = args[0], args[1], args[2]
    w_qkv, w_out, w_down, lm_head, fast_in = args[5], args[6], args[8], args[9], args[10]
    own_rows, width = stream_in.shape
    batch, ff = lengths.shape[0], w_down.shape[0]
    tp_count = lax.axis_size("tp")
    fits = (
        tp_count == 4 * QUAD
        and own_rows == 16
        and batch == 128
        and lax.axis_size("member") == 2
        and fast_in.shape[0] == 2
        and own_rows * tp_count == 2 * batch
        and w_qkv.shape[1] % HD == 0
        and w_out.shape[0] % HD == 0
        and w_qkv.shape[1] <= ff
        and width % 4096 == 0
        and kv_cache.shape[2] * 2 == width
        and lm_head.shape[1] == width
        and own_rows * kv_cache.shape[1] >= width + 2 * ff
    )
    if fits:
        return fused_body(*args)
    return plain_body(*args)


def solution(mesh):
    in_specs = (
        P(("member", "tp"), None),
        P(("member", "tp"), None, None),
        P(),
        P(),
        P(),
        P(None, "tp"),
        P("tp", None),
        P(None, None, "tp"),
        P("tp", None),
        P(None, "tp"),
        P("member", None, None),
        P("member", None, "tp"),
        P("member", None),
    )
    out_specs = (P(None, "tp"), P())
    return jax.shard_map(body, mesh=mesh, in_specs=in_specs, out_specs=out_specs, check_vma=False)
```
